1024 devices in a mesh: seq: 64 (over z, x), head: 16 (over y, core).
Axes of the slice: x: 4, y: 8, z: 16, core: 2. Of those that a mesh axis runs over, the one named last changes fastest.
Arguments:
- queries: bfloat16 [8192, 16, 64], P('seq', 'head'), may hold values from -6 to 6
- keys_values: bfloat16 [8192, 16, 128], P('seq', 'head'), may hold values from -6 to 6
- out_weight: bfloat16 [16, 64, 4096], P('head'), may hold values from -1 to 1
- out_grad: bfloat16 [8192, 4096], P('seq'), may hold values from -0.75 to 0.75
- block_order: int32 [64], replicated, may hold values from 0 to 63, each once
Outputs:
- mixed_out: bfloat16 [8192, 4096], P('seq', 'head')
- grad_queries: bfloat16 [8192, 16, 64], P('seq', 'head')
- grad_keys_values: bfloat16 [8192, 16, 128], P('seq', 'head')
The draws below stay inside these ranges and needn't reach their ends.
Inputs may be any that keep to these rules, and one draw needn't show every extreme that they name: `block_order`: A permutation of the sequence blocks 0 to 63.
All inputs are finite; a program needn't handle non-finite values.
Results may differ from the reference program's by a relative error of at most 0.03.
Values may be sent and summed in bfloat16 or wider, within the bound.
No kernel may reach another device: no remote copies, remote signals or barrier semaphores. Data moves between devices by JAX's collectives and lax.ppermute only.
A program may use at most 32 MiB of HBM per device.

```python
import math
import jax
import jax.numpy as jnp
from jax import lax

D = 4096
H = 16
HD = 64
TOK_DEV = 128
TOKENS = 8192
N_SEQ = 64


def drawn_normal(key):
    return jnp.clip(jax.random.normal(key, (TOKENS, H, HD), jnp.float32), -4.5, 4.5)


def draw_queries(key, part):
    return drawn_normal(jax.random.fold_in(key, 1)).astype(jnp.bfloat16)


def draw_keys_values(key, part):
    keys_part = drawn_normal(jax.random.fold_in(key, 2))
    values_part = drawn_normal(jax.random.fold_in(key, 3))
    return jnp.concatenate([keys_part, values_part], axis=2).astype(jnp.bfloat16)


def strengthened(entries, key, source, target, blocks, factor):
    def block_of(axis_at):
        return (jnp.arange(entries.shape[axis_at]) // (entries.shape[axis_at] // blocks)).reshape((-1,) + (1,) * (entries.ndim - 1 - axis_at))

    first = jax.random.permutation(key, blocks)[block_of(target)]
    second = (block_of(target) + blocks // 2) % blocks
    return jnp.where((block_of(source) == first) | (block_of(source) == second), factor * entries, entries)


def shard_levels(rng, extent, pieces, smallest, high):
    def one(dim, parts):
        steps = jax.random.uniform(jax.random.fold_in(jax.random.fold_in(rng, 6), dim), (parts,), jnp.float32, smallest / len(pieces), high / len(pieces))
        return jnp.repeat(jnp.exp(steps), extent[dim] // parts).reshape((-1,) + (1,) * (len(extent) - dim - 1))

    factor_of = one(*pieces[0])
    for cut in pieces[1:]:
        factor_of = factor_of * one(*cut)
    return factor_of


def normal_values(own_key, extent, width, most, cuts=(), kind=jnp.bfloat16):
    entries = jax.random.normal(own_key, extent, jnp.float32) * width
    if len(cuts) > 0:
        entries = shard_levels(own_key, extent, cuts, -0.22, 0.18) * entries
    return jnp.clip(entries, min=-most, max=most).astype(kind)


def gaussian_with(key, dims, scale, reach, cuts, heavy, held_as=jnp.bfloat16):
    drawn = scale * jax.random.normal(key, dims, jnp.float32)
    if cuts:
        drawn = drawn * shard_levels(key, dims, cuts, -0.22, 0.18)
    return jnp.clip(strengthened(drawn, jax.random.fold_in(key, 3), *heavy), -reach, reach).astype(held_as)


def setup_inputs(seed: int = 0) -> dict:
    seeds = jax.random.split(jax.random.key(seed), 6)
    return {
        "queries": draw_queries(jax.random.fold_in(seeds[5], 71), 0),
        "keys_values": draw_keys_values(jax.random.fold_in(seeds[5], 71), 0),
        "out_weight": gaussian_with(seeds[2], (H, HD, D), HD ** -0.5, 1.0, ((0, 16),), (0, 2, 16, 2.0)),
        "out_grad": normal_values(seeds[3], (TOKENS, D), 0.125, 0.75, ((0, 64),)),
        "block_order": jax.random.permutation(seeds[4], N_SEQ).astype(jnp.int32),
    }


def log_normalizer(scores, allowed):
    masked = jnp.where(allowed, scores, -jnp.inf)
    row_max = lax.optimization_barrier(jnp.max(masked, axis=-1, keepdims=True))
    row_total = lax.optimization_barrier(jnp.sum(jnp.exp(masked - row_max), axis=-1, keepdims=True))
    return row_max + jnp.log(row_total)

def reference(queries, keys_values, out_weight, out_grad, block_order):
    tok_index = jnp.arange(TOKENS, dtype=jnp.int32)
    position = block_order[tok_index // TOK_DEV] * TOK_DEV + tok_index % TOK_DEV
    allowed = position[None, :] <= position[:, None]
    inv_root = 1.0 / math.sqrt(HD)

    def one_head(carry, inputs):
        query_head, kv_head, weight_head = inputs
        key_head = kv_head[:, :HD]
        value_head = kv_head[:, HD:]
        scores = jnp.dot(query_head, key_head.T, preferred_element_type=jnp.float32) * inv_root
        log_total = log_normalizer(scores, allowed)
        probs_low = jnp.where(allowed, jnp.exp(scores - log_total), 0.0).astype(jnp.bfloat16)
        attended = jnp.dot(probs_low, value_head, preferred_element_type=jnp.float32).astype(jnp.bfloat16)
        carry = carry + jnp.dot(attended, weight_head, preferred_element_type=jnp.float32)
        grad_att = jnp.dot(out_grad, weight_head.T, preferred_element_type=jnp.float32).astype(jnp.bfloat16)
        grad_dot = lax.optimization_barrier(jnp.sum(grad_att.astype(jnp.float32) * attended.astype(jnp.float32), axis=1, keepdims=True))
        dprob = jnp.dot(grad_att, value_head.T, preferred_element_type=jnp.float32)
        dscore = (probs_low.astype(jnp.float32) * (dprob - grad_dot)).astype(jnp.bfloat16)
        grad_query = (jnp.dot(dscore, key_head, preferred_element_type=jnp.float32) * inv_root).astype(jnp.bfloat16)
        grad_key = jnp.dot(dscore.T, query_head, preferred_element_type=jnp.float32) * inv_root
        grad_value = jnp.dot(probs_low.T, grad_att, preferred_element_type=jnp.float32)
        grad_kv = jnp.concatenate([grad_key, grad_value], axis=1).astype(jnp.bfloat16)
        return (carry, (grad_query, grad_kv))
    start = jnp.zeros((TOKENS, D), jnp.float32)
    inputs = (jnp.transpose(queries, (1, 0, 2)), jnp.transpose(keys_values, (1, 0, 2)), out_weight)
    summed, stacked = lax.scan(one_head, start, inputs)
    grad_queries = jnp.transpose(stacked[0], (1, 0, 2))
    grad_keys_values = jnp.transpose(stacked[1], (1, 0, 2))
    return (summed.astype(jnp.bfloat16), grad_queries, grad_keys_values)
```

```python
import jax
import jax.numpy as jnp
from jax import lax
from jax.experimental import pallas as pl
from jax.experimental.pallas import tpu as pltpu
from jax.sharding import Mesh
from jax.sharding import PartitionSpec as P

GROUP = 8
SEQ = ("b", "a")
TOK = 128
HD = 64
ROWS = GROUP * TOK
STATS = 3 * GROUP
OUT_ROWS = HD + STATS
NEG = -1e30
INTERPRET = False
F32 = jnp.float32
BF16 = jnp.bfloat16


def nt(x, y):
    return lax.dot_general(x, y, (((1,), (1,)), ((), ())), preferred_element_type=F32)


def nn(x, y):
    return lax.dot_general(x, y, (((1,), (0,)), ((), ())), preferred_element_type=F32)


def lanes_below(x, flip=False):
    lane = lax.broadcasted_iota(jnp.int32, x.shape, x.ndim - 1)
    keep = lane >= HD if flip else lane < HD
    return jnp.where(keep, x, jnp.zeros_like(x))


def key_minus_query():
    key = lax.broadcasted_iota(jnp.int32, (TOK, TOK), 0)
    query = lax.broadcasted_iota(jnp.int32, (TOK, TOK), 1)
    return key - query


def forward_tile(order, place, qg_ref, kv_ref, out_ref, keys, values_t, stats):
    b, a = place[0], place[1]
    kv = kv_ref[...].reshape(ROWS, 2 * HD)
    keys[...] = lanes_below(kv)
    values_t[0:HD, :] = jnp.transpose(kv.astype(F32))[HD:, :].astype(BF16)
    values_t[HD:, :] = jnp.ones((16, ROWS), BF16)
    diff = key_minus_query()

    def step(i, carry):
        qg = qg_ref[i]
        scores = nt(keys[...], qg)
        query_block = order[b * GROUP + i]
        masked = []
        for j in range(GROUP):
            limit = (query_block - order[j * GROUP + a]) * TOK
            masked.append(jnp.where(diff <= limit, scores[j * TOK : (j + 1) * TOK], NEG))
        masked = jnp.concatenate(masked, axis=0)
        top = jnp.max(masked, axis=0, keepdims=True)
        probs = jnp.exp(masked - top).astype(BF16)
        summed = nn(values_t[...], probs)
        grad_t = jnp.transpose(qg.astype(F32))[HD:, :]
        part = summed[0:HD]
        out_ref[i, 0:HD, :] = part
        stats[pl.ds(i, 1), :] = top
        stats[pl.ds(GROUP + i, 1), :] = summed[HD : HD + 1]
        stats[pl.ds(2 * GROUP + i, 1), :] = jnp.sum(grad_t * part, axis=0, keepdims=True)
        return carry

    lax.fori_loop(0, GROUP, step, 0)
    for i in range(GROUP):
        out_ref[i, HD:, :] = stats[...]


def total_stats(parts_ref):
    top = parts_ref[0, HD : HD + GROUP, :]
    for p in range(1, GROUP):
        top = jnp.maximum(top, parts_ref[p, HD : HD + GROUP, :])
    total = jnp.zeros((GROUP, TOK), F32)
    dot = jnp.zeros((GROUP, TOK), F32)
    for p in range(GROUP):
        weight = jnp.exp(parts_ref[p, HD : HD + GROUP, :] - top)
        total += weight * parts_ref[p, HD + GROUP : HD + 2 * GROUP, :]
        dot += weight * parts_ref[p, HD + 2 * GROUP :, :]
    return top, total, dot / total


def join_parts(place, parts_ref, out_ref, tops, totals):
    a = place[1]
    top, total, _ = total_stats(parts_ref)
    tops[...] = top
    totals[...] = total
    own_top = tops[pl.ds(a, 1), :]
    own_total = totals[pl.ds(a, 1), :]
    acc = jnp.zeros((HD, TOK), F32)
    for p in range(GROUP):
        weight = jnp.exp(parts_ref[p, pl.ds(HD + a, 1), :] - own_top)
        acc += weight * parts_ref[p, 0:HD, :]
    out = (acc / own_total).astype(BF16)
    for h in range(out_ref.shape[0]):
        out_ref[h] = out


def backward_tile(
    order, place, qg_ref, kv_ref, parts_ref, dkv_ref, dq_ref, query_part, grad_part, dscores, norm_dot
):
    b, a = place[0], place[1]
    top, total, dot = total_stats(parts_ref)
    log_total = top + jnp.log(total)
    for i in range(GROUP):
        norm_dot[0:1, i * TOK : (i + 1) * TOK] = log_total[i : i + 1]
        norm_dot[1:2, i * TOK : (i + 1) * TOK] = dot[i : i + 1]
    qg = qg_ref[...].reshape(ROWS, 2 * HD)
    query_part[...] = lanes_below(qg)
    grad_part[...] = lanes_below(qg, True)
    diff = key_minus_query()

    def step(j, carry):
        kv = kv_ref[j]
        scores = nt(kv, query_part[...])
        dprob = nt(kv, grad_part[...])
        key_block = order[j * GROUP + a]
        logs = norm_dot[0:1, :]
        dots = norm_dot[1:2, :]
        allowed = jnp.concatenate(
            [diff <= (order[b * GROUP + i] - key_block) * TOK for i in range(GROUP)], axis=1
        )
        probs = jnp.where(allowed, jnp.exp(scores - logs), 0.0).astype(BF16)
        dscore = (probs.astype(F32) * (dprob - dots)).astype(BF16)
        dscores[pl.ds(pl.multiple_of(j * TOK, TOK), TOK), :] = dscore
        dkv = nn(dscore, query_part[...]) + nn(probs, grad_part[...])
        dkv_ref[j] = dkv.astype(BF16)
        return carry

    lax.fori_loop(0, GROUP, step, 0)
    keys_t = jnp.transpose(kv_ref[...].reshape(ROWS, 2 * HD).astype(F32))[0:HD, :].astype(BF16)
    dq = nn(keys_t, dscores[...]) * (HD**-0.5)
    for i in range(GROUP):
        dq_ref[i] = dq[:, i * TOK : (i + 1) * TOK].astype(BF16)


def smem():
    return pl.BlockSpec(memory_space=pltpu.SMEM)


def vmem():
    return pl.BlockSpec(memory_space=pltpu.VMEM)


def copies_for(value, axis):
    return jnp.broadcast_to(value[None], (lax.axis_size(axis), *value.shape))


def exchange(value, axis):
    return lax.all_to_all(value, axis, 0, 0, tiled=True)


def local(queries, keys_values, out_weight, out_grad, block_order):
    heads = lax.axis_size("head")
    place = jnp.stack([lax.axis_index("b"), lax.axis_index("a")]).astype(jnp.int32)
    kv_group = exchange(copies_for(keys_values[:, 0], "b"), "b")
    weight = out_weight[0]
    columns = weight.shape[1] // heads
    grad_att = lax.dot_general(
        out_grad, weight, (((1,), (1,)), ((), ())), preferred_element_type=F32
    ).astype(BF16)
    scaled = queries[:, 0] * jnp.asarray(HD**-0.5, BF16)
    qg_group = exchange(copies_for(jnp.concatenate([scaled, grad_att], axis=1), "a"), "a")
    column_weight = exchange(
        jnp.transpose(weight.reshape(HD, heads, columns), (1, 0, 2)), "head"
    )
    parts = pl.pallas_call(
        forward_tile,
        out_shape=jax.ShapeDtypeStruct((GROUP, OUT_ROWS, TOK), F32),
        in_specs=[smem(), smem(), vmem(), vmem()],
        out_specs=vmem(),
        scratch_shapes=[
            pltpu.VMEM((ROWS, 2 * HD), BF16),
            pltpu.VMEM((HD + 16, ROWS), BF16),
            pltpu.VMEM((STATS, TOK), F32),
        ],
        interpret=INTERPRET,
        name="forward_tile",
    )(block_order, place, qg_group, kv_group)
    parts = exchange(parts, "a")
    attended = pl.pallas_call(
        join_parts,
        out_shape=jax.ShapeDtypeStruct((heads, HD, TOK), BF16),
        in_specs=[smem(), vmem()],
        out_specs=vmem(),
        scratch_shapes=[pltpu.VMEM((GROUP, TOK), F32), pltpu.VMEM((GROUP, TOK), F32)],
        interpret=INTERPRET,
        name="join_parts",
    )(place, parts)
    every_head = exchange(attended, "head")
    dkv, dq = pl.pallas_call(
        backward_tile,
        out_shape=(
            jax.ShapeDtypeStruct((GROUP, TOK, 2 * HD), BF16),
            jax.ShapeDtypeStruct((GROUP, HD, TOK), BF16),
        ),
        in_specs=[smem(), smem(), vmem(), vmem(), vmem()],
        out_specs=(vmem(), vmem()),
        scratch_shapes=[
            pltpu.VMEM((ROWS, 2 * HD), BF16),
            pltpu.VMEM((ROWS, 2 * HD), BF16),
            pltpu.VMEM((ROWS, ROWS), BF16),
            pltpu.VMEM((8, ROWS), F32),
        ],
        interpret=INTERPRET,
        name="backward_tile",
    )(block_order, place, qg_group, kv_group, parts)
    dkv = exchange(dkv, "b")
    dq = exchange(dq, "a")
    grad_keys_values = jnp.sum(dkv.astype(F32), axis=0).astype(BF16)[:, None]
    grad_queries = jnp.transpose(jnp.sum(dq.astype(F32), axis=0)).astype(BF16)[:, None]
    mixed_out = lax.dot_general(
        every_head.reshape(heads * HD, TOK),
        column_weight.reshape(heads * HD, columns),
        (((0,), (0,)), ((), ())),
        preferred_element_type=F32,
    ).astype(BF16)
    return (mixed_out, grad_queries, grad_keys_values)


def solution(mesh):
    finer = Mesh(mesh.devices.reshape(GROUP, GROUP, mesh.shape["head"]), ("b", "a", "head"))
    in_specs = (
        P(SEQ, "head", None),
        P(SEQ, "head", None),
        P("head", None, None),
        P(SEQ, None),
        P(),
    )
    out_specs = (P(SEQ, "head"), P(SEQ, "head", None), P(SEQ, "head", None))
    return jax.shard_map(local, mesh=finer, in_specs=in_specs, out_specs=out_specs, check_vma=False)
```

```python
import jax
import jax.numpy as jnp
from jax import lax
from jax.experimental import pallas as pl
from jax.experimental.pallas import tpu as pltpu
from jax.sharding import Mesh
from jax.sharding import PartitionSpec as P

GROUP = 8
SEQ = ("b", "zl", "x")
TOK = 128
HD = 64
ROWS = GROUP * TOK
STATS = 3 * GROUP
QUARTERS = 4
A = ("zl", "x")
OUT_ROWS = HD + STATS
NEG = -1e30
INTERPRET = False
PARAMS = pltpu.CompilerParams(vmem_limit_bytes=24 * 1024 * 1024)
F32 = jnp.float32
BF16 = jnp.bfloat16


def nt(x, y):
    return lax.dot_general(x, y, (((1,), (1,)), ((), ())), preferred_element_type=F32)


def nn(x, y):
    return lax.dot_general(x, y, (((1,), (0,)), ((), ())), preferred_element_type=F32)


def lanes_below(x, flip=False):
    lane = lax.broadcasted_iota(jnp.int32, x.shape, x.ndim - 1)
    keep = lane >= HD if flip else lane < HD
    return jnp.where(keep, x, jnp.zeros_like(x))


def key_minus_query():
    key = lax.broadcasted_iota(jnp.int32, (TOK, TOK), 0)
    query = lax.broadcasted_iota(jnp.int32, (TOK, TOK), 1)
    return key - query


def forward_tile(order, place, qg_ref, kv_ref, out_ref, keys, values_t, stats):
    b, a = place[0], place[1]
    kv = kv_ref[...].reshape(ROWS, 2 * HD)
    keys[...] = lanes_below(kv)
    values_t[0:HD, :] = jnp.transpose(kv.astype(F32))[HD:, :].astype(BF16)
    values_t[HD:, :] = jnp.ones((16, ROWS), BF16)
    diff = key_minus_query()

    def step(i, carry):
        qg = qg_ref[i]
        scores = nt(keys[...], qg)
        query_block = order[b * GROUP + i]
        masked = []
        for j in range(GROUP):
            limit = (query_block - order[j * GROUP + a]) * TOK
            masked.append(jnp.where(diff <= limit, scores[j * TOK : (j + 1) * TOK], NEG))
        masked = jnp.concatenate(masked, axis=0)
        top = jnp.max(masked, axis=0, keepdims=True)
        probs = jnp.exp(masked - top).astype(BF16)
        summed = nn(values_t[...], probs)
        grad_t = jnp.transpose(qg.astype(F32))[HD:, :]
        part = summed[0:HD]
        out_ref[i, 0:HD, :] = part
        stats[pl.ds(i, 1), :] = top
        stats[pl.ds(GROUP + i, 1), :] = summed[HD : HD + 1]
        stats[pl.ds(2 * GROUP + i, 1), :] = jnp.sum(grad_t * part, axis=0, keepdims=True)
        return carry

    lax.fori_loop(0, GROUP, step, 0)
    for i in range(GROUP):
        out_ref[i, HD:, :] = stats[...]


def total_stats(parts_ref):
    top = parts_ref[0, HD : HD + GROUP, :]
    for p in range(1, GROUP):
        top = jnp.maximum(top, parts_ref[p, HD : HD + GROUP, :])
    total = jnp.zeros((GROUP, TOK), F32)
    dot = jnp.zeros((GROUP, TOK), F32)
    for p in range(GROUP):
        weight = jnp.exp(parts_ref[p, HD : HD + GROUP, :] - top)
        total += weight * parts_ref[p, HD + GROUP : HD + 2 * GROUP, :]
        dot += weight * parts_ref[p, HD + 2 * GROUP :, :]
    return top, total, dot / total


def prepare(queries_ref, weight_ref, grad_ref, out_ref):
    grad_att = nt(grad_ref[...], weight_ref[...]).astype(BF16)
    scaled = queries_ref[...] * jnp.asarray(HD**-0.5, BF16)
    out_ref[...] = jnp.concatenate([scaled, grad_att], axis=1)


def join_parts(place, parts_ref, weight_ref, out_ref, tops, totals):
    a, quarter = place[1], place[2]
    rows = HD // QUARTERS
    top, total, _ = total_stats(parts_ref)
    tops[...] = top
    totals[...] = total
    own_top = tops[pl.ds(a, 1), :]
    own_total = totals[pl.ds(a, 1), :]
    acc = jnp.zeros((HD, TOK), F32)
    for p in range(GROUP):
        weight = jnp.exp(parts_ref[p, pl.ds(HD + a, 1), :] - own_top)
        acc += weight * parts_ref[p, 0:HD, :]
    out = (acc / own_total).astype(BF16)
    for h in range(out_ref.shape[0]):
        out_ref[h, 0:HD, :] = out
    own_rows = weight_ref[pl.ds(pl.multiple_of(quarter * rows, rows), rows), :]
    for h in range(out_ref.shape[0]):
        for half in range(2):
            first = HD + half * rows
            column = (2 * h + half) * TOK
            out_ref[h, first : first + rows, :] = own_rows[:, column : column + TOK]


def mix(parts_ref, weight_ref, out_ref, side):
    heads = parts_ref.shape[0]
    rows = HD // QUARTERS
    for h in range(heads):
        for quarter in range(QUARTERS):
            first = h * HD + quarter * rows
            for half in range(2):
                side[first : first + rows, half * TOK : (half + 1) * TOK] = weight_ref[
                    quarter, h, half * rows : (half + 1) * rows, :
                ]
    attended = parts_ref[:, 0:HD, :].reshape(heads * HD, TOK)
    out_ref[...] = lax.dot_general(
        attended, side[...], (((0,), (0,)), ((), ())), preferred_element_type=F32
    ).astype(BF16)


def backward_tile(
    order, place, qg_ref, kv_ref, parts_ref, dkv_ref, dq_ref, query_part, grad_part, dscores, norm_dot
):
    b, a = place[0], place[1]
    top, total, dot = total_stats(parts_ref)
    log_total = top + jnp.log(total)
    for i in range(GROUP):
        norm_dot[0:1, i * TOK : (i + 1) * TOK] = log_total[i : i + 1]
        norm_dot[1:2, i * TOK : (i + 1) * TOK] = dot[i : i + 1]
    qg = qg_ref[...].reshape(ROWS, 2 * HD)
    query_part[...] = lanes_below(qg)
    grad_part[...] = lanes_below(qg, True)
    diff = key_minus_query()

    def step(j, carry):
        kv = kv_ref[j]
        scores = nt(kv, query_part[...])
        dprob = nt(kv, grad_part[...])
        key_block = order[j * GROUP + a]
        logs = norm_dot[0:1, :]
        dots = norm_dot[1:2, :]
        allowed = jnp.concatenate(
            [diff <= (order[b * GROUP + i] - key_block) * TOK for i in range(GROUP)], axis=1
        )
        probs = jnp.where(allowed, jnp.exp(scores - logs), 0.0).astype(BF16)
        dscore = (probs.astype(F32) * (dprob - dots)).astype(BF16)
        dscores[pl.ds(pl.multiple_of(j * TOK, TOK), TOK), :] = dscore
        dkv = nn(dscore, query_part[...]) + nn(probs, grad_part[...])
        dkv_ref[j] = dkv.astype(BF16)
        return carry

    lax.fori_loop(0, GROUP, step, 0)
    keys_t = jnp.transpose(kv_ref[...].reshape(ROWS, 2 * HD).astype(F32))[0:HD, :].astype(BF16)
    dq = nn(keys_t, dscores[...]) * (HD**-0.5)
    for i in range(GROUP):
        dq_ref[i] = dq[:, i * TOK : (i + 1) * TOK].astype(BF16)


def smem():
    return pl.BlockSpec(memory_space=pltpu.SMEM)


def vmem():
    return pl.BlockSpec(memory_space=pltpu.VMEM)


def copies_for(value, axis):
    return jnp.broadcast_to(value[None], (lax.axis_size(axis), *value.shape))


def exchange(value, axis):
    return lax.all_to_all(value, axis, 0, 0, tiled=True)


def local(queries, keys_values, out_weight, out_grad, block_order):
    heads = lax.axis_size("head")
    place = jnp.stack(
        [lax.axis_index("b"), lax.axis_index(A), lax.axis_index("x")]
    ).astype(jnp.int32)
    kv_group = exchange(copies_for(keys_values[:, 0], "b"), "b")
    weight = out_weight[0]
    columns = weight.shape[1] // heads
    query_grad = pl.pallas_call(
        prepare,
        out_shape=jax.ShapeDtypeStruct((TOK, 2 * HD), BF16),
        in_specs=[vmem(), vmem(), vmem()],
        out_specs=vmem(),
        interpret=INTERPRET,
        compiler_params=PARAMS,
        name="prepare",
    )(queries[:, 0], weight, out_grad)
    qg_group = lax.all_gather(lax.all_gather(query_grad, "x"), "zl")
    qg_group = qg_group.reshape(GROUP, TOK, 2 * HD)
    parts = pl.pallas_call(
        forward_tile,
        out_shape=jax.ShapeDtypeStruct((GROUP, OUT_ROWS, TOK), F32),
        in_specs=[smem(), smem(), vmem(), vmem()],
        out_specs=vmem(),
        scratch_shapes=[
            pltpu.VMEM((ROWS, 2 * HD), BF16),
            pltpu.VMEM((HD + 16, ROWS), BF16),
            pltpu.VMEM((STATS, TOK), F32),
        ],
        interpret=INTERPRET,
        compiler_params=PARAMS,
        name="forward_tile",
    )(block_order, place, qg_group, kv_group)
    parts = exchange(parts, A)
    mixed_parts = pl.pallas_call(
        join_parts,
        out_shape=jax.ShapeDtypeStruct((heads, HD + HD // QUARTERS * 2, TOK), BF16),
        in_specs=[smem(), vmem(), vmem()],
        out_specs=vmem(),
        scratch_shapes=[pltpu.VMEM((GROUP, TOK), F32), pltpu.VMEM((GROUP, TOK), F32)],
        interpret=INTERPRET,
        compiler_params=PARAMS,
        name="join_parts",
    )(place, parts, weight)
    mixed_parts = exchange(mixed_parts, "head")
    quarters = lax.all_gather(mixed_parts[:, HD:], "x")
    mixed_out = pl.pallas_call(
        mix,
        out_shape=jax.ShapeDtypeStruct((TOK, columns), BF16),
        in_specs=[vmem(), vmem()],
        out_specs=vmem(),
        scratch_shapes=[pltpu.VMEM((heads * HD, columns), BF16)],
        interpret=INTERPRET,
        compiler_params=PARAMS,
        name="mix",
    )(mixed_parts, quarters)
    dkv, dq = pl.pallas_call(
        backward_tile,
        out_shape=(
            jax.ShapeDtypeStruct((GROUP, TOK, 2 * HD), BF16),
            jax.ShapeDtypeStruct((GROUP, HD, TOK), BF16),
        ),
        in_specs=[smem(), smem(), vmem(), vmem(), vmem()],
        out_specs=(vmem(), vmem()),
        scratch_shapes=[
            pltpu.VMEM((ROWS, 2 * HD), BF16),
            pltpu.VMEM((ROWS, 2 * HD), BF16),
            pltpu.VMEM((ROWS, ROWS), BF16),
            pltpu.VMEM((8, ROWS), F32),
        ],
        interpret=INTERPRET,
        compiler_params=PARAMS,
        name="backward_tile",
    )(block_order, place, qg_group, kv_group, parts)
    dkv = exchange(dkv, "b")
    dq = exchange(dq, A)
    grad_keys_values = jnp.sum(dkv.astype(F32), axis=0).astype(BF16)[:, None]
    grad_queries = jnp.transpose(jnp.sum(dq.astype(F32), axis=0)).astype(BF16)[:, None]
    return (mixed_out, grad_queries, grad_keys_values)


def solution(mesh):
    finer = Mesh(mesh.devices.reshape(GROUP, 2, 4, mesh.shape["head"]), (*SEQ, "head"))
    in_specs = (
        P(SEQ, "head", None),
        P(SEQ, "head", None),
        P("head", None, None),
        P(SEQ, None),
        P(),
    )
    out_specs = (P(SEQ, "head"), P(SEQ, "head", None), P(SEQ, "head", None))
    return jax.shard_map(local, mesh=finer, in_specs=in_specs, out_specs=out_specs, check_vma=False)
```

```python
import jax
import jax.numpy as jnp
from jax import lax
from jax.experimental import pallas as pl
from jax.experimental.pallas import tpu as pltpu
from jax.sharding import Mesh
from jax.sharding import PartitionSpec as P

GROUP = 8
SEQ = ("b", "zl", "x")
TOK = 128
HD = 64
ROWS = GROUP * TOK
OUT, CENTRED, PLAIN, STATS = 0, HD, 2 * HD, 3 * HD
STAT_ROWS = 48
OUT_ROWS = STATS + STAT_ROWS
QUARTERS = 4
A = ("zl", "x")
NEG = -(2.0**100)
INTERPRET = False
PARAMS = pltpu.CompilerParams(vmem_limit_bytes=24 * 1024 * 1024)
F32 = jnp.float32
BF16 = jnp.bfloat16


def nt(x, y):
    return lax.dot_general(x, y, (((1,), (1,)), ((), ())), preferred_element_type=F32)


def nn(x, y):
    return lax.dot_general(x, y, (((1,), (0,)), ((), ())), preferred_element_type=F32)


def lanes_below(x, flip=False):
    lane = lax.broadcasted_iota(jnp.int32, x.shape, x.ndim - 1)
    keep = lane >= HD if flip else lane < HD
    return jnp.where(keep, x, jnp.zeros_like(x))


def key_minus_query():
    key = lax.broadcasted_iota(jnp.int32, (TOK, TOK), 0)
    query = lax.broadcasted_iota(jnp.int32, (TOK, TOK), 1)
    return key - query


def split(value):
    high = value.astype(BF16).astype(F32)
    return high, value - high


def forward_tile(order, place, qg_ref, kv_ref, out_ref, keys, values, kv_t, stats):
    b, a = place[0], place[1]
    kv = kv_ref[...].reshape(ROWS, 2 * HD)
    keys[...] = lanes_below(kv)
    values[...] = lanes_below(kv, True)
    kv_t[0 : 2 * HD, :] = jnp.transpose(kv.astype(F32)).astype(BF16)
    kv_t[2 * HD :, :] = jnp.ones((16, ROWS), BF16)
    stats[...] = jnp.zeros((STAT_ROWS, TOK), F32)
    diff = key_minus_query()

    def step(i, carry):
        qg = qg_ref[i]
        scores = nt(keys[...], qg)
        query_block = order[b * GROUP + i]
        masked = []
        for j in range(GROUP):
            limit = (query_block - order[j * GROUP + a]) * TOK
            masked.append(jnp.where(diff <= limit, scores[j * TOK : (j + 1) * TOK], NEG))
        masked = jnp.concatenate(masked, axis=0)
        top = jnp.max(masked, axis=0, keepdims=True).astype(BF16).astype(F32)
        probs = jnp.exp(masked - top).astype(BF16)
        summed = nn(kv_t[...], probs)
        grad_t = jnp.transpose(qg.astype(F32))[HD:, :]
        part = summed[HD : 2 * HD]
        total = summed[2 * HD : 2 * HD + 1]
        dot = jnp.sum(grad_t * part, axis=0, keepdims=True)
        dprob = nt(values[...], qg)
        dscore = (probs.astype(F32) * (dprob - dot / total)).astype(BF16)
        out_ref[i, OUT : OUT + HD, :] = part.astype(BF16)
        out_ref[i, CENTRED : CENTRED + HD, :] = nn(kv_t[0:HD, :], dscore).astype(BF16)
        out_ref[i, PLAIN : PLAIN + HD, :] = summed[0:HD].astype(BF16)
        rows = (top, *split(total), *split(dot))
        for k, row in enumerate(rows):
            stats[pl.ds(k * GROUP + i, 1), :] = row
        return carry

    lax.fori_loop(0, GROUP, step, 0)
    for i in range(GROUP):
        out_ref[i, STATS:, :] = stats[...].astype(BF16)


def part_stats(parts_ref):
    tops, totals, dots = [], [], []
    for p in range(GROUP):
        rows = parts_ref[p, STATS:, :].astype(F32)
        tops.append(rows[0:GROUP])
        totals.append(rows[GROUP : 2 * GROUP] + rows[2 * GROUP : 3 * GROUP])
        dots.append(rows[3 * GROUP : 4 * GROUP] + rows[4 * GROUP : 5 * GROUP])
    return tops, totals, dots


def joined(tops, totals, dots):
    top = tops[0]
    for p in range(1, GROUP):
        top = jnp.maximum(top, tops[p])
    weights = [jnp.exp(tops[p] - top) for p in range(GROUP)]
    total = sum(weights[p] * totals[p] for p in range(GROUP))
    dot = sum(weights[p] * dots[p] for p in range(GROUP))
    return top, total, dot / total, weights


def prepare(queries_hbm, weight_hbm, grad_hbm, out_ref, queries_t, weight, grad, sems):
    pairs = ((queries_hbm, queries_t), (weight_hbm, weight), (grad_hbm, grad))
    loads = [pltpu.make_async_copy(*pair, sems.at[k]) for k, pair in enumerate(pairs)]
    for load in loads:
        load.start()
    for load in loads:
        load.wait()
    grad_att = nt(grad[...], weight[...])
    scaled = jnp.transpose(queries_t[...].astype(F32)) * HD**-0.5
    out_ref[...] = jnp.concatenate([scaled, grad_att], axis=1).astype(BF16)


def join_parts(place, parts_ref, weight_ref, out_ref, dq_ref, own):
    a, quarter = place[1], place[2]
    rows = HD // QUARTERS
    tops, totals, dots = part_stats(parts_ref)
    _, total, dot, weights = joined(tops, totals, dots)
    own[0:GROUP, :] = 1.0 / total
    for p in range(GROUP):
        shift = dot - dots[p] / totals[p]
        own[(2 * p + 1) * GROUP : (2 * p + 2) * GROUP, :] = weights[p]
        own[(2 * p + 2) * GROUP : (2 * p + 3) * GROUP, :] = weights[p] * shift
    attended = jnp.zeros((HD, TOK), F32)
    dq = jnp.zeros((HD, TOK), F32)
    for p in range(GROUP):
        weight = own[pl.ds((2 * p + 1) * GROUP + a, 1), :]
        shifted = own[pl.ds((2 * p + 2) * GROUP + a, 1), :]
        attended += weight * parts_ref[p, OUT : OUT + HD, :].astype(F32)
        dq += weight * parts_ref[p, CENTRED : CENTRED + HD, :].astype(F32)
        dq -= shifted * parts_ref[p, PLAIN : PLAIN + HD, :].astype(F32)
    scale = own[pl.ds(a, 1), :]
    dq_ref[...] = (dq * (scale * HD**-0.5)).astype(BF16)
    out = (attended * scale).astype(BF16)
    for h in range(out_ref.shape[0]):
        out_ref[h, 0:HD, :] = out
    own_rows = weight_ref[pl.ds(pl.multiple_of(quarter * rows, rows), rows), :]
    for h in range(out_ref.shape[0]):
        for half in range(2):
            first = HD + half * rows
            column = (2 * h + half) * TOK
            out_ref[h, first : first + rows, :] = own_rows[:, column : column + TOK]


def mix(parts_ref, weight_ref, out_ref, side):
    heads = parts_ref.shape[0]
    rows = HD // QUARTERS
    for h in range(heads):
        for quarter in range(QUARTERS):
            first = h * HD + quarter * rows
            for half in range(2):
                side[first : first + rows, half * TOK : (half + 1) * TOK] = weight_ref[
                    quarter, h, half * rows : (half + 1) * rows, :
                ]
    attended = parts_ref[:, 0:HD, :].reshape(heads * HD, TOK)
    out_ref[...] = lax.dot_general(
        attended, side[...], (((0,), (0,)), ((), ())), preferred_element_type=F32
    ).astype(BF16)


def backward_tile(
    order, place, qg_ref, kv_ref, parts_ref, dkv_ref, query_part, grad_part, norm_dot
):
    b, a = place[0], place[1]
    top, total, dot, _ = joined(*part_stats(parts_ref))
    log_total = top + jnp.log(total)
    for i in range(GROUP):
        norm_dot[0:1, i * TOK : (i + 1) * TOK] = log_total[i : i + 1]
        norm_dot[1:2, i * TOK : (i + 1) * TOK] = dot[i : i + 1]
    qg = qg_ref[...].reshape(ROWS, 2 * HD)
    query_part[...] = lanes_below(qg)
    grad_part[...] = lanes_below(qg, True)
    diff = key_minus_query()

    def step(j, carry):
        kv = kv_ref[j]
        scores = nt(kv, query_part[...])
        dprob = nt(kv, grad_part[...])
        key_block = order[j * GROUP + a]
        logs = norm_dot[0:1, :]
        dots = norm_dot[1:2, :]
        allowed = jnp.concatenate(
            [diff <= (order[b * GROUP + i] - key_block) * TOK for i in range(GROUP)], axis=1
        )
        probs = jnp.where(allowed, jnp.exp(scores - logs), 0.0).astype(BF16)
        dscore = (probs.astype(F32) * (dprob - dots)).astype(BF16)
        dkv = nn(dscore, query_part[...]) + nn(probs, grad_part[...])
        dkv_ref[j] = dkv.astype(BF16)
        return carry

    lax.fori_loop(0, GROUP, step, 0)


def smem():
    return pl.BlockSpec(memory_space=pltpu.SMEM)


def vmem():
    return pl.BlockSpec(memory_space=pltpu.VMEM)


def copies_for(value, axis):
    return jnp.broadcast_to(value[None], (lax.axis_size(axis), *value.shape))


def exchange(value, axis):
    return lax.all_to_all(value, axis, 0, 0, tiled=True)


def local(queries, keys_values, out_weight, out_grad, block_order):
    heads = lax.axis_size("head")
    place = jnp.stack(
        [lax.axis_index("b"), lax.axis_index(A), lax.axis_index("x")]
    ).astype(jnp.int32)
    kv_group = exchange(copies_for(keys_values[:, 0], "b"), "b")
    weight = out_weight[0]
    columns = weight.shape[1] // heads
    query_grad = pl.pallas_call(
        prepare,
        out_shape=jax.ShapeDtypeStruct((TOK, 2 * HD), BF16),
        in_specs=[pl.BlockSpec(memory_space=pltpu.HBM)] * 3,
        out_specs=vmem(),
        scratch_shapes=[
            pltpu.VMEM((HD, TOK), BF16),
            pltpu.VMEM(weight.shape, BF16),
            pltpu.VMEM(out_grad.shape, BF16),
            pltpu.SemaphoreType.DMA((3,)),
        ],
        interpret=INTERPRET,
        compiler_params=PARAMS,
        name="prepare",
    )(jnp.transpose(queries[:, 0]), weight, out_grad)
    qg_group = lax.all_gather(lax.all_gather(query_grad, "x"), "zl")
    qg_group = qg_group.reshape(GROUP, TOK, 2 * HD)
    parts = pl.pallas_call(
        forward_tile,
        out_shape=jax.ShapeDtypeStruct((GROUP, OUT_ROWS, TOK), BF16),
        in_specs=[smem(), smem(), vmem(), vmem()],
        out_specs=vmem(),
        scratch_shapes=[
            pltpu.VMEM((ROWS, 2 * HD), BF16),
            pltpu.VMEM((ROWS, 2 * HD), BF16),
            pltpu.VMEM((2 * HD + 16, ROWS), BF16),
            pltpu.VMEM((STAT_ROWS, TOK), F32),
        ],
        interpret=INTERPRET,
        compiler_params=PARAMS,
        name="forward_tile",
    )(block_order, place, qg_group, kv_group)
    parts = exchange(parts, A)
    mixed_parts, grad_queries = pl.pallas_call(
        join_parts,
        out_shape=(
            jax.ShapeDtypeStruct((heads, HD + HD // QUARTERS * 2, TOK), BF16),
            jax.ShapeDtypeStruct((HD, TOK), BF16),
        ),
        in_specs=[smem(), vmem(), vmem()],
        out_specs=(vmem(), vmem()),
        scratch_shapes=[pltpu.VMEM(((2 * GROUP + 1) * GROUP, TOK), F32)],
        interpret=INTERPRET,
        compiler_params=PARAMS,
        name="join_parts",
    )(place, parts, weight)
    mixed_parts = exchange(mixed_parts, "head")
    quarters = lax.all_gather(mixed_parts[:, HD:], "x")
    mixed_out = pl.pallas_call(
        mix,
        out_shape=jax.ShapeDtypeStruct((TOK, columns), BF16),
        in_specs=[vmem(), vmem()],
        out_specs=vmem(),
        scratch_shapes=[pltpu.VMEM((heads * HD, columns), BF16)],
        interpret=INTERPRET,
        compiler_params=PARAMS,
        name="mix",
    )(mixed_parts, quarters)
    dkv = pl.pallas_call(
        backward_tile,
        out_shape=jax.ShapeDtypeStruct((GROUP, TOK, 2 * HD), BF16),
        in_specs=[smem(), smem(), vmem(), vmem(), vmem()],
        out_specs=vmem(),
        scratch_shapes=[
            pltpu.VMEM((ROWS, 2 * HD), BF16),
            pltpu.VMEM((ROWS, 2 * HD), BF16),
            pltpu.VMEM((8, ROWS), F32),
        ],
        interpret=INTERPRET,
        compiler_params=PARAMS,
        name="backward_tile",
    )(block_order, place, qg_group, kv_group, parts)
    dkv = exchange(dkv, "b")
    grad_keys_values = jnp.sum(dkv.astype(F32), axis=0).astype(BF16)[:, None]
    return (mixed_out, jnp.transpose(grad_queries)[:, None], grad_keys_values)


def solution(mesh):
    finer = Mesh(mesh.devices.reshape(GROUP, 2, 4, mesh.shape["head"]), (*SEQ, "head"))
    in_specs = (
        P(SEQ, "head", None),
        P(SEQ, "head", None),
        P("head", None, None),
        P(SEQ, None),
        P(),
    )
    out_specs = (P(SEQ, "head"), P(SEQ, "head", None), P(SEQ, "head", None))
    return jax.shard_map(local, mesh=finer, in_specs=in_specs, out_specs=out_specs, check_vma=False)
```

```python
import jax
import jax.numpy as jnp
from jax import lax
from jax.experimental import pallas as pl
from jax.experimental.pallas import tpu as pltpu
from jax.sharding import Mesh
from jax.sharding import PartitionSpec as P

GROUP = 8
SEQ = ("b", "zl", "x")
TOK = 128
HD = 64
ROWS = GROUP * TOK
OUT, CENTRED, PLAIN, STATS = 0, HD, 2 * HD, 3 * HD
STAT_ROWS = 48
OUT_ROWS = STATS + STAT_ROWS
QUARTERS = 4
WIDE = 4
A = ("zl", "x")
NEG = -(2.0**100)
INTERPRET = False
PARAMS = pltpu.CompilerParams(vmem_limit_bytes=24 * 1024 * 1024)
F32 = jnp.float32
BF16 = jnp.bfloat16


def nt(x, y):
    return lax.dot_general(x, y, (((1,), (1,)), ((), ())), preferred_element_type=F32)


def nn(x, y):
    return lax.dot_general(x, y, (((1,), (0,)), ((), ())), preferred_element_type=F32)


def lanes_below(x, flip=False):
    lane = lax.broadcasted_iota(jnp.int32, x.shape, x.ndim - 1)
    keep = lane >= HD if flip else lane < HD
    return jnp.where(keep, x, jnp.zeros_like(x))


def fill_caps(caps):
    key = lax.broadcasted_iota(jnp.int32, (TOK, TOK), 0)
    query = lax.broadcasted_iota(jnp.int32, (TOK, TOK), 1)
    caps[0:TOK, :] = jnp.full((TOK, TOK), NEG, F32)
    caps[TOK : 2 * TOK, :] = jnp.where(key <= query, -NEG, NEG)
    caps[2 * TOK :, :] = jnp.full((TOK, TOK), -NEG, F32)


def cap_for(caps, key_block, query_block):
    later = jnp.clip(query_block - key_block, -1, 1) + 1
    return caps[pl.ds(pl.multiple_of(later * TOK, TOK), TOK), :]


def split(value):
    high = value.astype(BF16).astype(F32)
    return high, value - high


def forward_tile(order, place, qg_ref, kv_ref, out_ref, keys, values, kv_t, stats, caps):
    b, a = place[0], place[1]
    kv = kv_ref[...].reshape(ROWS, 2 * HD)
    keys[...] = lanes_below(kv)
    values[...] = lanes_below(kv, True)
    kv_t[0 : 2 * HD, :] = jnp.transpose(kv.astype(F32)).astype(BF16)
    kv_t[2 * HD :, :] = jnp.ones((16, ROWS), BF16)
    stats[...] = jnp.zeros((STAT_ROWS, TOK), F32)
    fill_caps(caps)
    for first in range(0, GROUP, WIDE):
        blocks = range(first, first + WIDE)
        qg = qg_ref[first : first + WIDE].reshape(WIDE * TOK, 2 * HD)
        scores = nt(keys[...], qg)
        masked = []
        for j in range(GROUP):
            key_block = order[j * GROUP + a]
            cap = jnp.concatenate(
                [cap_for(caps, key_block, order[b * GROUP + i]) for i in blocks], axis=1
            )
            masked.append(jnp.minimum(scores[j * TOK : (j + 1) * TOK], cap))
        masked = jnp.concatenate(masked, axis=0)
        top = jnp.max(masked, axis=0, keepdims=True).astype(BF16).astype(F32)
        probs = jnp.exp(masked - top).astype(BF16)
        summed = nn(kv_t[...], probs)
        grad_t = jnp.transpose(qg.astype(F32))[HD:, :]
        part = summed[HD : 2 * HD]
        total = summed[2 * HD : 2 * HD + 1]
        dot = jnp.sum(grad_t * part, axis=0, keepdims=True)
        dprob = nt(values[...], qg)
        dscore = probs * (dprob - dot / total).astype(BF16)
        centred = nn(kv_t[0:HD, :], dscore)
        rows = (top, *split(total), *split(dot))
        for i in blocks:
            lanes = slice((i - first) * TOK, (i - first + 1) * TOK)
            out_ref[i, OUT : OUT + HD, :] = part[:, lanes].astype(BF16)
            out_ref[i, CENTRED : CENTRED + HD, :] = centred[:, lanes].astype(BF16)
            out_ref[i, PLAIN : PLAIN + HD, :] = summed[0:HD, lanes].astype(BF16)
            for k, row in enumerate(rows):
                stats[k * GROUP + i : k * GROUP + i + 1, :] = row[:, lanes]
    for i in range(GROUP):
        out_ref[i, STATS:, :] = stats[...].astype(BF16)


def part_stats(parts_ref):
    tops, totals, dots = [], [], []
    for p in range(GROUP):
        rows = parts_ref[p, STATS:, :].astype(F32)
        tops.append(rows[0:GROUP])
        totals.append(rows[GROUP : 2 * GROUP] + rows[2 * GROUP : 3 * GROUP])
        dots.append(rows[3 * GROUP : 4 * GROUP] + rows[4 * GROUP : 5 * GROUP])
    return tops, totals, dots


def joined(tops, totals, dots):
    top = tops[0]
    for p in range(1, GROUP):
        top = jnp.maximum(top, tops[p])
    weights = [jnp.exp(tops[p] - top) for p in range(GROUP)]
    total = sum(weights[p] * totals[p] for p in range(GROUP))
    dot = sum(weights[p] * dots[p] for p in range(GROUP))
    return top, total, dot / total, weights


def prepare(
    queries_hbm, kv_hbm, weight_hbm, grad_hbm, qg_ref, copies_ref, queries_t, kv, weight, grad, sems
):
    pairs = ((kv_hbm, kv), (weight_hbm, weight), (grad_hbm, grad), (queries_hbm, queries_t))
    loads = [pltpu.make_async_copy(*pair, sems.at[k]) for k, pair in enumerate(pairs)]
    for load in loads:
        load.start()
    loads[0].wait()
    for p in range(GROUP):
        copies_ref[p] = kv[...]
    for load in loads[1:]:
        load.wait()
    grad_att = nt(grad[...], weight[...])
    scaled = jnp.transpose(queries_t[...].astype(F32)) * HD**-0.5
    qg_ref[...] = jnp.concatenate([scaled, grad_att], axis=1).astype(BF16)


def join_parts(place, parts_ref, weight_ref, out_ref, dq_ref, own):
    a, quarter = place[1], place[2]
    rows = HD // QUARTERS
    tops, totals, dots = part_stats(parts_ref)
    _, total, dot, weights = joined(tops, totals, dots)
    own[0:GROUP, :] = 1.0 / total
    for p in range(GROUP):
        shift = dot - dots[p] / totals[p]
        own[(2 * p + 1) * GROUP : (2 * p + 2) * GROUP, :] = weights[p]
        own[(2 * p + 2) * GROUP : (2 * p + 3) * GROUP, :] = weights[p] * shift
    attended = jnp.zeros((HD, TOK), F32)
    dq = jnp.zeros((HD, TOK), F32)
    for p in range(GROUP):
        weight = own[pl.ds((2 * p + 1) * GROUP + a, 1), :]
        shifted = own[pl.ds((2 * p + 2) * GROUP + a, 1), :]
        attended += weight * parts_ref[p, OUT : OUT + HD, :].astype(F32)
        dq += weight * parts_ref[p, CENTRED : CENTRED + HD, :].astype(F32)
        dq -= shifted * parts_ref[p, PLAIN : PLAIN + HD, :].astype(F32)
    scale = own[pl.ds(a, 1), :]
    dq_ref[...] = (dq * (scale * HD**-0.5)).astype(BF16)
    out = (attended * scale).astype(BF16)
    for h in range(out_ref.shape[0]):
        out_ref[h, 0:HD, :] = out
    own_rows = weight_ref[pl.ds(pl.multiple_of(quarter * rows, rows), rows), :]
    for h in range(out_ref.shape[0]):
        for half in range(2):
            first = HD + half * rows
            column = (2 * h + half) * TOK
            out_ref[h, first : first + rows, :] = own_rows[:, column : column + TOK]


def mix(parts_ref, weight_ref, out_ref, side):
    heads = parts_ref.shape[0]
    rows = HD // QUARTERS
    for h in range(heads):
        for quarter in range(QUARTERS):
            first = h * HD + quarter * rows
            for half in range(2):
                side[first : first + rows, half * TOK : (half + 1) * TOK] = weight_ref[
                    quarter, h, half * rows : (half + 1) * rows, :
                ]
    attended = parts_ref[:, 0:HD, :].reshape(heads * HD, TOK)
    out_ref[...] = lax.dot_general(
        attended, side[...], (((0,), (0,)), ((), ())), preferred_element_type=F32
    ).astype(BF16)


def backward_tile(
    order, place, qg_ref, kv_ref, parts_ref, dkv_ref, query_part, grad_part, norm_dot, caps
):
    b, a = place[0], place[1]
    top, total, dot, _ = joined(*part_stats(parts_ref))
    log_total = top + jnp.log(total)
    for i in range(GROUP):
        norm_dot[0:1, i * TOK : (i + 1) * TOK] = log_total[i : i + 1]
        norm_dot[1:2, i * TOK : (i + 1) * TOK] = dot[i : i + 1]
    qg = qg_ref[...].reshape(ROWS, 2 * HD)
    query_part[...] = lanes_below(qg)
    grad_part[...] = lanes_below(qg, True)
    fill_caps(caps)
    for j in range(GROUP):
        kv = kv_ref[j]
        key_block = order[j * GROUP + a]
        cap = jnp.concatenate(
            [cap_for(caps, key_block, order[b * GROUP + i]) for i in range(GROUP)], axis=1
        )
        masked = jnp.minimum(nt(kv, query_part[...]), cap)
        probs = jnp.exp(masked - norm_dot[0:1, :]).astype(BF16)
        dprob = nt(kv, grad_part[...])
        dscore = probs * (dprob - norm_dot[1:2, :]).astype(BF16)
        dkv = nn(dscore, query_part[...]) + nn(probs, grad_part[...])
        dkv_ref[j] = dkv.astype(BF16)


def smem():
    return pl.BlockSpec(memory_space=pltpu.SMEM)


def vmem():
    return pl.BlockSpec(memory_space=pltpu.VMEM)


def exchange(value, axis):
    return lax.all_to_all(value, axis, 0, 0, tiled=True)


def local(queries, keys_values, out_weight, out_grad, block_order):
    heads = lax.axis_size("head")
    place = jnp.stack(
        [lax.axis_index("b"), lax.axis_index(A), lax.axis_index("x")]
    ).astype(jnp.int32)
    weight = out_weight[0]
    columns = weight.shape[1] // heads
    query_grad, kv_copies = pl.pallas_call(
        prepare,
        out_shape=(
            jax.ShapeDtypeStruct((TOK, 2 * HD), BF16),
            jax.ShapeDtypeStruct((GROUP, TOK, 2 * HD), BF16),
        ),
        in_specs=[pl.BlockSpec(memory_space=pltpu.HBM)] * 4,
        out_specs=(vmem(), vmem()),
        scratch_shapes=[
            pltpu.VMEM((HD, TOK), BF16),
            pltpu.VMEM((TOK, 2 * HD), BF16),
            pltpu.VMEM(weight.shape, BF16),
            pltpu.VMEM(out_grad.shape, BF16),
            pltpu.SemaphoreType.DMA((4,)),
        ],
        interpret=INTERPRET,
        name="prepare",
    )(jnp.transpose(queries[:, 0]), keys_values[:, 0], weight, out_grad)
    kv_group = exchange(kv_copies, "b")
    qg_group = query_grad
    for pairs in ([[0, 1], [2, 3]], [[0, 3], [1, 2]]):
        qg_group = lax.all_gather(qg_group, "x", tiled=True, axis_index_groups=pairs)
    qg_group = lax.all_gather(qg_group, "zl")
    qg_group = qg_group.reshape(GROUP, TOK, 2 * HD)
    parts = pl.pallas_call(
        forward_tile,
        out_shape=jax.ShapeDtypeStruct((GROUP, OUT_ROWS, TOK), BF16),
        in_specs=[smem(), smem(), vmem(), vmem()],
        out_specs=vmem(),
        scratch_shapes=[
            pltpu.VMEM((ROWS, 2 * HD), BF16),
            pltpu.VMEM((ROWS, 2 * HD), BF16),
            pltpu.VMEM((2 * HD + 16, ROWS), BF16),
            pltpu.VMEM((STAT_ROWS, TOK), F32),
            pltpu.VMEM((3 * TOK, TOK), F32),
        ],
        interpret=INTERPRET,
        compiler_params=PARAMS,
        name="forward_tile",
    )(block_order, place, qg_group, kv_group)
    parts = exchange(parts, A)
    mixed_parts, grad_queries = pl.pallas_call(
        join_parts,
        out_shape=(
            jax.ShapeDtypeStruct((heads, HD + HD // QUARTERS * 2, TOK), BF16),
            jax.ShapeDtypeStruct((HD, TOK), BF16),
        ),
        in_specs=[smem(), vmem(), vmem()],
        out_specs=(vmem(), vmem()),
        scratch_shapes=[pltpu.VMEM(((2 * GROUP + 1) * GROUP, TOK), F32)],
        interpret=INTERPRET,
        compiler_params=PARAMS,
        name="join_parts",
    )(place, parts, weight)
    mixed_parts = exchange(mixed_parts, "head")
    quarters = lax.all_gather(mixed_parts[:, HD:], "x")
    mixed_out = pl.pallas_call(
        mix,
        out_shape=jax.ShapeDtypeStruct((TOK, columns), BF16),
        in_specs=[vmem(), vmem()],
        out_specs=vmem(),
        scratch_shapes=[pltpu.VMEM((heads * HD, columns), BF16)],
        interpret=INTERPRET,
        compiler_params=PARAMS,
        name="mix",
    )(mixed_parts, quarters)
    dkv = pl.pallas_call(
        backward_tile,
        out_shape=jax.ShapeDtypeStruct((GROUP, TOK, 2 * HD), BF16),
        in_specs=[smem(), smem(), vmem(), vmem(), vmem()],
        out_specs=vmem(),
        scratch_shapes=[
            pltpu.VMEM((ROWS, 2 * HD), BF16),
            pltpu.VMEM((ROWS, 2 * HD), BF16),
            pltpu.VMEM((8, ROWS), F32),
            pltpu.VMEM((3 * TOK, TOK), F32),
        ],
        interpret=INTERPRET,
        compiler_params=PARAMS,
        name="backward_tile",
    )(block_order, place, qg_group, kv_group, parts)
    dkv = exchange(dkv, "b")
    grad_keys_values = jnp.sum(dkv.astype(F32), axis=0).astype(BF16)[:, None]
    return (mixed_out, jnp.transpose(grad_queries)[:, None], grad_keys_values)


def solution(mesh):
    finer = Mesh(mesh.devices.reshape(GROUP, 2, 4, mesh.shape["head"]), (*SEQ, "head"))
    in_specs = (
        P(SEQ, "head", None),
        P(SEQ, "head", None),
        P("head", None, None),
        P(SEQ, None),
        P(),
    )
    out_specs = (P(SEQ, "head"), P(SEQ, "head", None), P(SEQ, "head", None))
    return jax.shard_map(local, mesh=finer, in_specs=in_specs, out_specs=out_specs, check_vma=False)
```

```python
import jax
import jax.numpy as jnp
from jax import lax
from jax.experimental import pallas as pl
from jax.experimental.pallas import tpu as pltpu
from jax.sharding import Mesh
from jax.sharding import PartitionSpec as P

GROUP = 8
SEQ = ("b", "zl", "x")
TOK = 128
HD = 64
ROWS = GROUP * TOK
OUT, CENTRED, PLAIN, STATS = 0, HD, 2 * HD, 3 * HD
STAT_ROWS = 48
OUT_ROWS = STATS + STAT_ROWS
QUARTERS = 4
WIDE = 8
A = ("zl", "x")
GATHERED = [(g % 2) * 4 + g // 2 for g in range(GROUP)]
B_AT, A_AT, X_AT = 64, 65, 66
NEG = -(2.0**100)
INTERPRET = False
PARAMS = pltpu.CompilerParams(vmem_limit_bytes=24 * 1024 * 1024)
F32 = jnp.float32
BF16 = jnp.bfloat16


def nt(x, y):
    return lax.dot_general(x, y, (((1,), (1,)), ((), ())), preferred_element_type=F32)


def nn(x, y):
    return lax.dot_general(x, y, (((1,), (0,)), ((), ())), preferred_element_type=F32)


def lanes_below(x, flip=False):
    lane = lax.broadcasted_iota(jnp.int32, x.shape, x.ndim - 1)
    keep = lane >= HD if flip else lane < HD
    return jnp.where(keep, x, jnp.zeros_like(x))


def fill_caps(caps):
    key = lax.broadcasted_iota(jnp.int32, (TOK, TOK), 0)
    query = lax.broadcasted_iota(jnp.int32, (TOK, TOK), 1)
    caps[0:TOK, :] = jnp.full((TOK, TOK), NEG, F32)
    caps[TOK : 2 * TOK, :] = jnp.where(key <= query, -NEG, NEG)
    caps[2 * TOK :, :] = jnp.full((TOK, TOK), -NEG, F32)


def cap_for(caps, key_block, query_block):
    later = jnp.clip(query_block - key_block, -1, 1) + 1
    return caps[pl.ds(pl.multiple_of(later * TOK, TOK), TOK), :]


def split(value):
    high = value.astype(BF16).astype(F32)
    return high, value - high


def forward_tile(order, qg_ref, kv_ref, out_ref, keys, values, kv_t, stats, caps):
    b, a = order[B_AT], order[A_AT]
    kv = kv_ref[...].reshape(ROWS, 2 * HD)
    keys[...] = lanes_below(kv)
    values[...] = lanes_below(kv, True)
    kv_t[0 : 2 * HD, :] = jnp.transpose(kv.astype(F32)).astype(BF16)
    kv_t[2 * HD :, :] = jnp.ones((16, ROWS), BF16)
    stats[...] = jnp.zeros((STAT_ROWS, TOK), F32)
    fill_caps(caps)
    for first in range(0, GROUP, WIDE):
        blocks = range(first, first + WIDE)
        qg = qg_ref[first : first + WIDE].reshape(WIDE * TOK, 2 * HD)
        scores = nt(keys[...], qg)
        masked = []
        for j in range(GROUP):
            key_block = order[j * GROUP + a]
            cap = jnp.concatenate(
                [cap_for(caps, key_block, order[b * GROUP + GATHERED[g]]) for g in blocks], axis=1
            )
            masked.append(jnp.minimum(scores[j * TOK : (j + 1) * TOK], cap))
        masked = jnp.concatenate(masked, axis=0)
        top = jnp.max(masked, axis=0, keepdims=True).astype(BF16).astype(F32)
        probs = jnp.exp(masked - top).astype(BF16)
        summed = nn(kv_t[...], probs)
        grad_t = jnp.transpose(qg.astype(F32))[HD:, :]
        part = summed[HD : 2 * HD]
        total = summed[2 * HD : 2 * HD + 1]
        dot = jnp.sum(grad_t * part, axis=0, keepdims=True)
        dprob = nt(values[...], qg)
        dscore = probs * (dprob - dot / total).astype(BF16)
        centred = nn(kv_t[0:HD, :], dscore)
        rows = (top, *split(total), *split(dot))
        for g in blocks:
            i = GATHERED[g]
            lanes = slice((g - first) * TOK, (g - first + 1) * TOK)
            out_ref[i, OUT : OUT + HD, :] = part[:, lanes].astype(BF16)
            out_ref[i, CENTRED : CENTRED + HD, :] = centred[:, lanes].astype(BF16)
            out_ref[i, PLAIN : PLAIN + HD, :] = summed[0:HD, lanes].astype(BF16)
            for k, row in enumerate(rows):
                stats[k * GROUP + i : k * GROUP + i + 1, :] = row[:, lanes]
    for i in range(GROUP):
        out_ref[i, STATS:, :] = stats[...].astype(BF16)


def part_stats(parts_ref):
    tops, totals, dots = [], [], []
    for p in range(GROUP):
        rows = parts_ref[p, STATS:, :].astype(F32)
        tops.append(rows[0:GROUP])
        totals.append(rows[GROUP : 2 * GROUP] + rows[2 * GROUP : 3 * GROUP])
        dots.append(rows[3 * GROUP : 4 * GROUP] + rows[4 * GROUP : 5 * GROUP])
    return tops, totals, dots


def joined(tops, totals, dots):
    top = tops[0]
    for p in range(1, GROUP):
        top = jnp.maximum(top, tops[p])
    weights = [jnp.exp(tops[p] - top) for p in range(GROUP)]
    total = sum(weights[p] * totals[p] for p in range(GROUP))
    dot = sum(weights[p] * dots[p] for p in range(GROUP))
    return top, total, dot / total, weights


def prepare(
    queries_hbm, kv_hbm, weight_hbm, grad_hbm, qg_ref, copies_ref, queries_t, kv, weight, grad, sems
):
    pairs = ((kv_hbm, kv), (weight_hbm, weight), (grad_hbm, grad), (queries_hbm, queries_t))
    loads = [pltpu.make_async_copy(*pair, sems.at[k]) for k, pair in enumerate(pairs)]
    for load in loads:
        load.start()
    loads[0].wait()
    for p in range(GROUP):
        copies_ref[p] = kv[...]
    for load in loads[1:]:
        load.wait()
    grad_att = nt(grad[...], weight[...])
    scaled = jnp.transpose(queries_t[...].astype(F32)) * HD**-0.5
    qg_ref[...] = jnp.concatenate([scaled, grad_att], axis=1).astype(BF16)


def join_parts(order, parts_ref, weight_ref, out_ref, own):
    a, quarter = order[A_AT], order[X_AT]
    rows = HD // QUARTERS
    tops, totals, dots = part_stats(parts_ref)
    _, total, _, weights = joined(tops, totals, dots)
    for p in range(GROUP):
        own[p * GROUP : (p + 1) * GROUP, :] = weights[p] / total
    attended = jnp.zeros((HD, TOK), F32)
    for p in range(GROUP):
        weight = own[pl.ds(p * GROUP + a, 1), :]
        attended += weight * parts_ref[p, OUT : OUT + HD, :].astype(F32)
    out = attended.astype(BF16)
    for h in range(out_ref.shape[0]):
        out_ref[h, 0:HD, :] = out
    own_rows = weight_ref[pl.ds(pl.multiple_of(quarter * rows, rows), rows), :]
    for h in range(out_ref.shape[0]):
        for half in range(2):
            first = HD + half * rows
            column = (2 * h + half) * TOK
            out_ref[h, first : first + rows, :] = own_rows[:, column : column + TOK]


def mix(order, parts_ref, mixed_ref, weight_ref, out_ref, dq_ref, side, own):
    a = order[A_AT]
    tops, totals, dots = part_stats(parts_ref)
    _, total, dot, weights = joined(tops, totals, dots)
    for p in range(GROUP):
        scaled = weights[p] / total * HD**-0.5
        own[2 * p * GROUP : (2 * p + 1) * GROUP, :] = scaled
        own[(2 * p + 1) * GROUP : (2 * p + 2) * GROUP, :] = scaled * (dot - dots[p] / totals[p])
    dq = jnp.zeros((HD, TOK), F32)
    for p in range(GROUP):
        weight = own[pl.ds(2 * p * GROUP + a, 1), :]
        shifted = own[pl.ds((2 * p + 1) * GROUP + a, 1), :]
        dq += weight * parts_ref[p, CENTRED : CENTRED + HD, :].astype(F32)
        dq -= shifted * parts_ref[p, PLAIN : PLAIN + HD, :].astype(F32)
    dq_ref[...] = dq.astype(BF16)
    heads = mixed_ref.shape[0]
    rows = HD // QUARTERS
    for h in range(heads):
        for quarter in range(QUARTERS):
            first = h * HD + quarter * rows
            for half in range(2):
                side[first : first + rows, half * TOK : (half + 1) * TOK] = weight_ref[
                    quarter, h, half * rows : (half + 1) * rows, :
                ]
    attended = mixed_ref[:, 0:HD, :].reshape(heads * HD, TOK)
    out_ref[...] = lax.dot_general(
        attended, side[...], (((0,), (0,)), ((), ())), preferred_element_type=F32
    ).astype(BF16)


def backward_tile(
    order, qg_ref, kv_ref, parts_ref, dkv_ref, query_part, grad_part, norm_dot, caps
):
    b, a = order[B_AT], order[A_AT]
    top, total, dot, _ = joined(*part_stats(parts_ref))
    log_total = top + jnp.log(total)
    for g, i in enumerate(GATHERED):
        norm_dot[0:1, g * TOK : (g + 1) * TOK] = log_total[i : i + 1]
        norm_dot[1:2, g * TOK : (g + 1) * TOK] = dot[i : i + 1]
    qg = qg_ref[...].reshape(ROWS, 2 * HD)
    query_part[...] = lanes_below(qg)
    grad_part[...] = lanes_below(qg, True)
    fill_caps(caps)
    for j in range(GROUP):
        kv = kv_ref[j]
        key_block = order[j * GROUP + a]
        cap = jnp.concatenate(
            [cap_for(caps, key_block, order[b * GROUP + i]) for i in GATHERED], axis=1
        )
        masked = jnp.minimum(nt(kv, query_part[...]), cap)
        probs = jnp.exp(masked - norm_dot[0:1, :]).astype(BF16)
        dprob = nt(kv, grad_part[...])
        dscore = probs * (dprob - norm_dot[1:2, :]).astype(BF16)
        dkv = nn(dscore, query_part[...]) + nn(probs, grad_part[...])
        dkv_ref[j] = dkv.astype(BF16)


def smem():
    return pl.BlockSpec(memory_space=pltpu.SMEM)


def vmem():
    return pl.BlockSpec(memory_space=pltpu.VMEM)


def exchange(value, axis):
    return lax.all_to_all(value, axis, 0, 0, tiled=True)


def local(queries, keys_values, out_weight, out_grad, block_order):
    heads = lax.axis_size("head")
    place = [lax.axis_index("b"), lax.axis_index(A), lax.axis_index("x")]
    order = jnp.concatenate([block_order, jnp.stack(place).astype(jnp.int32)])
    weight = out_weight[0]
    columns = weight.shape[1] // heads
    query_grad, kv_copies = pl.pallas_call(
        prepare,
        out_shape=(
            jax.ShapeDtypeStruct((TOK, 2 * HD), BF16),
            jax.ShapeDtypeStruct((GROUP, TOK, 2 * HD), BF16),
        ),
        in_specs=[pl.BlockSpec(memory_space=pltpu.HBM)] * 4,
        out_specs=(vmem(), vmem()),
        scratch_shapes=[
            pltpu.VMEM((HD, TOK), BF16),
            pltpu.VMEM((TOK, 2 * HD), BF16),
            pltpu.VMEM(weight.shape, BF16),
            pltpu.VMEM(out_grad.shape, BF16),
            pltpu.SemaphoreType.DMA((4,)),
        ],
        interpret=INTERPRET,
        name="prepare",
    )(jnp.transpose(queries[:, 0]), keys_values[:, 0], weight, out_grad)
    kv_group = exchange(kv_copies, "b")
    qg_group = lax.all_gather(query_grad, "zl", tiled=True)
    for pairs in ([[0, 1], [2, 3]], [[0, 3], [1, 2]]):
        qg_group = lax.all_gather(qg_group, "x", tiled=True, axis_index_groups=pairs)
    qg_group = qg_group.reshape(GROUP, TOK, 2 * HD)
    parts = pl.pallas_call(
        forward_tile,
        out_shape=jax.ShapeDtypeStruct((GROUP, OUT_ROWS, TOK), BF16),
        in_specs=[smem(), vmem(), vmem()],
        out_specs=vmem(),
        scratch_shapes=[
            pltpu.VMEM((ROWS, 2 * HD), BF16),
            pltpu.VMEM((ROWS, 2 * HD), BF16),
            pltpu.VMEM((2 * HD + 16, ROWS), BF16),
            pltpu.VMEM((STAT_ROWS, TOK), F32),
            pltpu.VMEM((3 * TOK, TOK), F32),
        ],
        interpret=INTERPRET,
        compiler_params=PARAMS,
        name="forward_tile",
    )(order, qg_group, kv_group)
    parts = exchange(parts, A)
    mixed_parts = pl.pallas_call(
        join_parts,
        out_shape=jax.ShapeDtypeStruct((heads, HD + HD // QUARTERS * 2, TOK), BF16),
        in_specs=[smem(), vmem(), vmem()],
        out_specs=vmem(),
        scratch_shapes=[pltpu.VMEM((GROUP * GROUP, TOK), F32)],
        interpret=INTERPRET,
        compiler_params=PARAMS,
        name="join_parts",
    )(order, parts, weight)
    mixed_parts = exchange(mixed_parts, "head")
    quarters = lax.all_gather(mixed_parts[:, HD:], "x")
    mixed_out, grad_queries = pl.pallas_call(
        mix,
        out_shape=(
            jax.ShapeDtypeStruct((TOK, columns), BF16),
            jax.ShapeDtypeStruct((HD, TOK), BF16),
        ),
        in_specs=[smem(), vmem(), vmem(), vmem()],
        out_specs=(vmem(), vmem()),
        scratch_shapes=[
            pltpu.VMEM((heads * HD, columns), BF16),
            pltpu.VMEM((2 * GROUP * GROUP, TOK), F32),
        ],
        interpret=INTERPRET,
        compiler_params=PARAMS,
        name="mix",
    )(order, parts, mixed_parts, quarters)
    dkv = pl.pallas_call(
        backward_tile,
        out_shape=jax.ShapeDtypeStruct((GROUP, TOK, 2 * HD), BF16),
        in_specs=[smem(), vmem(), vmem(), vmem()],
        out_specs=vmem(),
        scratch_shapes=[
            pltpu.VMEM((ROWS, 2 * HD), BF16),
            pltpu.VMEM((ROWS, 2 * HD), BF16),
            pltpu.VMEM((8, ROWS), F32),
            pltpu.VMEM((3 * TOK, TOK), F32),
        ],
        interpret=INTERPRET,
        compiler_params=PARAMS,
        name="backward_tile",
    )(order, qg_group, kv_group, parts)
    dkv = exchange(dkv, "b")
    grad_keys_values = jnp.sum(dkv.astype(F32), axis=0).astype(BF16)[:, None]
    return (mixed_out, jnp.transpose(grad_queries)[:, None], grad_keys_values)


def solution(mesh):
    finer = Mesh(mesh.devices.reshape(GROUP, 2, 4, mesh.shape["head"]), (*SEQ, "head"))
    in_specs = (
        P(SEQ, "head", None),
        P(SEQ, "head", None),
        P("head", None, None),
        P(SEQ, None),
        P(),
    )
    out_specs = (P(SEQ, "head"), P(SEQ, "head", None), P(SEQ, "head", None))
    return jax.shard_map(local, mesh=finer, in_specs=in_specs, out_specs=out_specs, check_vma=False)
```

```python
import jax
import jax.numpy as jnp
from jax import lax
from jax.experimental import pallas as pl
from jax.experimental.pallas import tpu as pltpu
from jax.sharding import Mesh
from jax.sharding import PartitionSpec as P

GROUP = 8
SEQ = ("b", "zl", "x")
TOK = 128
HD = 64
ROWS = GROUP * TOK
OUT, CENTRED, PLAIN, STATS = 0, HD, 2 * HD, 3 * HD
STAT_ROWS = 48
OUT_ROWS = STATS + STAT_ROWS
QUARTERS = 4
WIDE = 8
A = ("zl", "x")
HEAD = ("y", "c")
GATHERED = range(GROUP)
B_AT, A_AT, X_AT = 64, 65, 66
NEG = -(2.0**100)
INTERPRET = False
PARAMS = pltpu.CompilerParams(vmem_limit_bytes=24 * 1024 * 1024)
F32 = jnp.float32
BF16 = jnp.bfloat16


def nt(x, y):
    return lax.dot_general(x, y, (((1,), (1,)), ((), ())), preferred_element_type=F32)


def nn(x, y):
    return lax.dot_general(x, y, (((1,), (0,)), ((), ())), preferred_element_type=F32)


def lanes_below(x, flip=False):
    lane = lax.broadcasted_iota(jnp.int32, x.shape, x.ndim - 1)
    keep = lane >= HD if flip else lane < HD
    return jnp.where(keep, x, jnp.zeros_like(x))


def fill_caps(caps):
    key = lax.broadcasted_iota(jnp.int32, (TOK, TOK), 0)
    query = lax.broadcasted_iota(jnp.int32, (TOK, TOK), 1)
    caps[0:TOK, :] = jnp.full((TOK, TOK), NEG, F32)
    caps[TOK : 2 * TOK, :] = jnp.where(key <= query, -NEG, NEG)
    caps[2 * TOK :, :] = jnp.full((TOK, TOK), -NEG, F32)


def cap_for(caps, key_block, query_block):
    later = jnp.clip(query_block - key_block, -1, 1) + 1
    return caps[pl.ds(pl.multiple_of(later * TOK, TOK), TOK), :]


def split(value):
    high = value.astype(BF16).astype(F32)
    return high, value - high


def forward_tile(order, qg_ref, kv_ref, out_ref, keys, values, kv_t, stats, caps):
    b, a = order[B_AT], order[A_AT]
    kv = kv_ref[...].reshape(ROWS, 2 * HD)
    keys[...] = lanes_below(kv)
    values[...] = lanes_below(kv, True)
    kv_t[0 : 2 * HD, :] = jnp.transpose(kv.astype(F32)).astype(BF16)
    kv_t[2 * HD :, :] = jnp.ones((16, ROWS), BF16)
    stats[...] = jnp.zeros((STAT_ROWS, TOK), F32)
    fill_caps(caps)
    for first in range(0, GROUP, WIDE):
        blocks = range(first, first + WIDE)
        qg = qg_ref[first : first + WIDE].reshape(WIDE * TOK, 2 * HD)
        scores = nt(keys[...], qg)
        masked = []
        for j in range(GROUP):
            key_block = order[j * GROUP + a]
            cap = jnp.concatenate(
                [cap_for(caps, key_block, order[b * GROUP + GATHERED[g]]) for g in blocks], axis=1
            )
            masked.append(jnp.minimum(scores[j * TOK : (j + 1) * TOK], cap))
        masked = jnp.concatenate(masked, axis=0)
        top = jnp.max(masked, axis=0, keepdims=True).astype(BF16).astype(F32)
        probs = jnp.exp(masked - top).astype(BF16)
        summed = nn(kv_t[...], probs)
        grad_t = jnp.transpose(qg.astype(F32))[HD:, :]
        part = summed[HD : 2 * HD]
        total = summed[2 * HD : 2 * HD + 1]
        dot = jnp.sum(grad_t * part, axis=0, keepdims=True)
        dprob = nt(values[...], qg)
        dscore = probs * (dprob - dot / total).astype(BF16)
        centred = nn(kv_t[0:HD, :], dscore)
        rows = (top, *split(total), *split(dot))
        for g in blocks:
            i = GATHERED[g]
            lanes = slice((g - first) * TOK, (g - first + 1) * TOK)
            out_ref[i, OUT : OUT + HD, :] = part[:, lanes].astype(BF16)
            out_ref[i, CENTRED : CENTRED + HD, :] = centred[:, lanes].astype(BF16)
            out_ref[i, PLAIN : PLAIN + HD, :] = summed[0:HD, lanes].astype(BF16)
            for k, row in enumerate(rows):
                stats[k * GROUP + i : k * GROUP + i + 1, :] = row[:, lanes]
    for i in range(GROUP):
        out_ref[i, STATS:, :] = stats[...].astype(BF16)


def part_stats(parts_ref):
    tops, totals, dots = [], [], []
    for p in range(GROUP):
        rows = parts_ref[p, STATS:, :].astype(F32)
        tops.append(rows[0:GROUP])
        totals.append(rows[GROUP : 2 * GROUP] + rows[2 * GROUP : 3 * GROUP])
        dots.append(rows[3 * GROUP : 4 * GROUP] + rows[4 * GROUP : 5 * GROUP])
    return tops, totals, dots


def joined(tops, totals, dots):
    top = tops[0]
    for p in range(1, GROUP):
        top = jnp.maximum(top, tops[p])
    weights = [jnp.exp(tops[p] - top) for p in range(GROUP)]
    total = sum(weights[p] * totals[p] for p in range(GROUP))
    dot = sum(weights[p] * dots[p] for p in range(GROUP))
    return top, total, dot / total, weights


def prepare(
    queries_hbm, kv_hbm, weight_hbm, grad_hbm, qg_ref, copies_ref, queries_t, kv, weight, grad, sems
):
    pairs = ((kv_hbm, kv), (weight_hbm, weight), (grad_hbm, grad), (queries_hbm, queries_t))
    loads = [pltpu.make_async_copy(*pair, sems.at[k]) for k, pair in enumerate(pairs)]
    for load in loads:
        load.start()
    loads[0].wait()
    for p in range(GROUP):
        copies_ref[p] = kv[...]
    for load in loads[1:]:
        load.wait()
    grad_att = nt(grad[...], weight[...])
    scaled = jnp.transpose(queries_t[...].astype(F32)) * HD**-0.5
    qg_ref[...] = jnp.concatenate([scaled, grad_att], axis=1).astype(BF16)


def join_parts(order, parts_ref, weight_ref, out_ref, own):
    a, quarter = order[A_AT], order[X_AT]
    rows = HD // QUARTERS
    tops, totals, dots = part_stats(parts_ref)
    _, total, _, weights = joined(tops, totals, dots)
    for p in range(GROUP):
        own[p * GROUP : (p + 1) * GROUP, :] = weights[p] / total
    attended = jnp.zeros((HD, TOK), F32)
    for p in range(GROUP):
        weight = own[pl.ds(p * GROUP + a, 1), :]
        attended += weight * parts_ref[p, OUT : OUT + HD, :].astype(F32)
    out = attended.astype(BF16)
    own_rows = weight_ref[pl.ds(pl.multiple_of(quarter * rows, rows), rows), :]
    for y in range(out_ref.shape[0]):
        out_ref[y, 0:HD, :] = out
        for k in range(4):
            first = HD + k * rows
            column = (4 * y + k) * TOK
            out_ref[y, first : first + rows, :] = own_rows[:, column : column + TOK]


def mix(order, parts_ref, mixed_ref, weight_ref, out_ref, dq_ref, side, own):
    a = order[A_AT]
    tops, totals, dots = part_stats(parts_ref)
    _, total, dot, weights = joined(tops, totals, dots)
    for p in range(GROUP):
        scaled = weights[p] / total * HD**-0.5
        own[2 * p * GROUP : (2 * p + 1) * GROUP, :] = scaled
        own[(2 * p + 1) * GROUP : (2 * p + 2) * GROUP, :] = scaled * (dot - dots[p] / totals[p])
    dq = jnp.zeros((HD, TOK), F32)
    for p in range(GROUP):
        weight = own[pl.ds(2 * p * GROUP + a, 1), :]
        shifted = own[pl.ds((2 * p + 1) * GROUP + a, 1), :]
        dq += weight * parts_ref[p, CENTRED : CENTRED + HD, :].astype(F32)
        dq -= shifted * parts_ref[p, PLAIN : PLAIN + HD, :].astype(F32)
    dq_ref[...] = dq.astype(BF16)
    cores, chips = mixed_ref.shape[:2]
    rows = HD // QUARTERS
    for c in range(cores):
        for y in range(chips):
            for quarter in range(QUARTERS):
                first = (c * chips + y) * HD + quarter * rows
                for half in range(2):
                    side[first : first + rows, half * TOK : (half + 1) * TOK] = weight_ref[
                        quarter, c, y, half * rows : (half + 1) * rows, :
                    ]
    attended = mixed_ref[:, :, 0:HD, :].reshape(cores * chips * HD, TOK)
    out_ref[...] = lax.dot_general(
        attended, side[...], (((0,), (0,)), ((), ())), preferred_element_type=F32
    ).astype(BF16)


def backward_tile(
    order, qg_ref, kv_ref, parts_ref, dkv_ref, query_part, grad_part, norm_dot, caps
):
    b, a = order[B_AT], order[A_AT]
    top, total, dot, _ = joined(*part_stats(parts_ref))
    log_total = top + jnp.log(total)
    for g, i in enumerate(GATHERED):
        norm_dot[0:1, g * TOK : (g + 1) * TOK] = log_total[i : i + 1]
        norm_dot[1:2, g * TOK : (g + 1) * TOK] = dot[i : i + 1]
    qg = qg_ref[...].reshape(ROWS, 2 * HD)
    query_part[...] = lanes_below(qg)
    grad_part[...] = lanes_below(qg, True)
    fill_caps(caps)
    for j in range(GROUP):
        kv = kv_ref[j]
        key_block = order[j * GROUP + a]
        cap = jnp.concatenate(
            [cap_for(caps, key_block, order[b * GROUP + i]) for i in GATHERED], axis=1
        )
        masked = jnp.minimum(nt(kv, query_part[...]), cap)
        probs = jnp.exp(masked - norm_dot[0:1, :]).astype(BF16)
        dprob = nt(kv, grad_part[...])
        dscore = probs * (dprob - norm_dot[1:2, :]).astype(BF16)
        dkv = nn(dscore, query_part[...]) + nn(probs, grad_part[...])
        dkv_ref[j] = dkv.astype(BF16)


def smem():
    return pl.BlockSpec(memory_space=pltpu.SMEM)


def vmem():
    return pl.BlockSpec(memory_space=pltpu.VMEM)


def exchange(value, axis):
    return lax.all_to_all(value, axis, 0, 0, tiled=True)


def local(queries, keys_values, out_weight, out_grad, block_order):
    chips = lax.axis_size("y")
    heads = chips * lax.axis_size("c")
    place = [lax.axis_index(name) for name in ("b", A, "x")]
    order = jnp.concatenate([block_order, jnp.stack(place).astype(jnp.int32)])
    weight = out_weight[0]
    columns = weight.shape[1] // heads
    query_grad, kv_copies = pl.pallas_call(
        prepare,
        out_shape=(
            jax.ShapeDtypeStruct((TOK, 2 * HD), BF16),
            jax.ShapeDtypeStruct((GROUP, TOK, 2 * HD), BF16),
        ),
        in_specs=[pl.BlockSpec(memory_space=pltpu.HBM)] * 4,
        out_specs=(vmem(), vmem()),
        scratch_shapes=[
            pltpu.VMEM((HD, TOK), BF16),
            pltpu.VMEM((TOK, 2 * HD), BF16),
            pltpu.VMEM(weight.shape, BF16),
            pltpu.VMEM(out_grad.shape, BF16),
            pltpu.SemaphoreType.DMA((4,)),
        ],
        interpret=INTERPRET,
        name="prepare",
    )(jnp.transpose(queries[:, 0]), keys_values[:, 0], weight, out_grad)
    kv_group = exchange(kv_copies, "b")
    qg_group = query_grad
    for pairs in ([[0, 1], [2, 3]], [[0, 3], [1, 2]]):
        qg_group = lax.all_gather(qg_group, "x", tiled=True, axis_index_groups=pairs)
    qg_group = lax.all_gather(qg_group, "zl")
    qg_group = qg_group.reshape(GROUP, TOK, 2 * HD)
    parts = pl.pallas_call(
        forward_tile,
        out_shape=jax.ShapeDtypeStruct((GROUP, OUT_ROWS, TOK), BF16),
        in_specs=[smem(), vmem(), vmem()],
        out_specs=vmem(),
        scratch_shapes=[
            pltpu.VMEM((ROWS, 2 * HD), BF16),
            pltpu.VMEM((ROWS, 2 * HD), BF16),
            pltpu.VMEM((2 * HD + 16, ROWS), BF16),
            pltpu.VMEM((STAT_ROWS, TOK), F32),
            pltpu.VMEM((3 * TOK, TOK), F32),
        ],
        interpret=INTERPRET,
        compiler_params=PARAMS,
        name="forward_tile",
    )(order, qg_group, kv_group)
    parts = exchange(parts, A)
    mixed_parts = pl.pallas_call(
        join_parts,
        out_shape=jax.ShapeDtypeStruct((chips, 2 * HD, TOK), BF16),
        in_specs=[smem(), vmem(), vmem()],
        out_specs=vmem(),
        scratch_shapes=[pltpu.VMEM((GROUP * GROUP, TOK), F32)],
        interpret=INTERPRET,
        compiler_params=PARAMS,
        name="join_parts",
    )(order, parts, weight)
    mixed_parts = exchange(mixed_parts, "y")
    every_head = lax.all_gather(mixed_parts, "c")
    own_side = 2 * HD // QUARTERS
    quarters = lax.dynamic_slice_in_dim(
        every_head, HD + lax.axis_index("c") * own_side, own_side, axis=2
    )
    quarters = lax.all_gather(quarters, "x")
    mixed_out, grad_queries = pl.pallas_call(
        mix,
        out_shape=(
            jax.ShapeDtypeStruct((TOK, columns), BF16),
            jax.ShapeDtypeStruct((HD, TOK), BF16),
        ),
        in_specs=[smem(), vmem(), vmem(), vmem()],
        out_specs=(vmem(), vmem()),
        scratch_shapes=[
            pltpu.VMEM((heads * HD, columns), BF16),
            pltpu.VMEM((2 * GROUP * GROUP, TOK), F32),
        ],
        interpret=INTERPRET,
        compiler_params=PARAMS,
        name="mix",
    )(order, parts, every_head, quarters)
    dkv = pl.pallas_call(
        backward_tile,
        out_shape=jax.ShapeDtypeStruct((GROUP, TOK, 2 * HD), BF16),
        in_specs=[smem(), vmem(), vmem(), vmem()],
        out_specs=vmem(),
        scratch_shapes=[
            pltpu.VMEM((ROWS, 2 * HD), BF16),
            pltpu.VMEM((ROWS, 2 * HD), BF16),
            pltpu.VMEM((8, ROWS), F32),
            pltpu.VMEM((3 * TOK, TOK), F32),
        ],
        interpret=INTERPRET,
        compiler_params=PARAMS,
        name="backward_tile",
    )(order, qg_group, kv_group, parts)
    dkv = exchange(dkv, "b")
    grad_keys_values = jnp.sum(dkv.astype(F32), axis=0).astype(BF16)[:, None]
    return (mixed_out, jnp.transpose(grad_queries)[:, None], grad_keys_values)


def solution(mesh):
    finer = Mesh(mesh.devices.reshape(GROUP, 2, 4, mesh.shape["head"] // 2, 2), (*SEQ, *HEAD))
    in_specs = (
        P(SEQ, HEAD, None),
        P(SEQ, HEAD, None),
        P(HEAD, None, None),
        P(SEQ, None),
        P(),
    )
    out_specs = (P(SEQ, HEAD), P(SEQ, HEAD, None), P(SEQ, HEAD, None))
    return jax.shard_map(local, mesh=finer, in_specs=in_specs, out_specs=out_specs, check_vma=False)
```

```python
import jax
import jax.numpy as jnp
from jax import lax
from jax.experimental import pallas as pl
from jax.experimental.pallas import tpu as pltpu
from jax.sharding import Mesh
from jax.sharding import PartitionSpec as P

GROUP = 8
SEQ = ("b", "zl", "x")
TOK = 128
HD = 64
ROWS = GROUP * TOK
OUT, CENTRED, PLAIN, STATS = 0, HD, 2 * HD, 3 * HD
STAT_ROWS = 32
OUT_ROWS = STATS + STAT_ROWS
QUARTERS = 4
WIDE = 8
A = ("zl", "x")
HEAD = ("y", "c")
GATHERED = range(GROUP)
B_AT, A_AT, X_AT = 64, 65, 66
NEG = -(2.0**100)
INTERPRET = False
PARAMS = pltpu.CompilerParams(vmem_limit_bytes=24 * 1024 * 1024)
F32 = jnp.float32
BF16 = jnp.bfloat16


def nt(x, y):
    return lax.dot_general(x, y, (((1,), (1,)), ((), ())), preferred_element_type=F32)


def nn(x, y):
    return lax.dot_general(x, y, (((1,), (0,)), ((), ())), preferred_element_type=F32)


def lanes_below(x, flip=False):
    lane = lax.broadcasted_iota(jnp.int32, x.shape, x.ndim - 1)
    keep = lane >= HD if flip else lane < HD
    return jnp.where(keep, x, jnp.zeros_like(x))


def fill_caps(caps):
    key = lax.broadcasted_iota(jnp.int32, (TOK, TOK), 0)
    query = lax.broadcasted_iota(jnp.int32, (TOK, TOK), 1)
    caps[0:TOK, :] = jnp.full((TOK, TOK), NEG, F32)
    caps[TOK : 2 * TOK, :] = jnp.where(key <= query, -NEG, NEG)
    caps[2 * TOK :, :] = jnp.full((TOK, TOK), -NEG, F32)


def cap_for(caps, key_block, query_block):
    later = jnp.clip(query_block - key_block, -1, 1) + 1
    return caps[pl.ds(pl.multiple_of(later * TOK, TOK), TOK), :]


def split(value):
    high = value.astype(BF16).astype(F32)
    return high, value - high


def forward_tile(order, qg_ref, kv_ref, out_ref, keys, values, kv_t, stats, caps):
    b, a = order[B_AT], order[A_AT]
    kv = kv_ref[...].reshape(ROWS, 2 * HD)
    keys[...] = lanes_below(kv)
    values[...] = lanes_below(kv, True)
    kv_t[0 : 2 * HD, :] = jnp.transpose(kv.astype(F32)).astype(BF16)
    kv_t[2 * HD :, :] = jnp.ones((16, ROWS), BF16)
    stats[...] = jnp.zeros((STAT_ROWS, TOK), F32)
    fill_caps(caps)
    for first in range(0, GROUP, WIDE):
        blocks = range(first, first + WIDE)
        qg = qg_ref[first : first + WIDE].reshape(WIDE * TOK, 2 * HD)
        scores = nt(keys[...], qg)
        masked = []
        for j in range(GROUP):
            key_block = order[j * GROUP + a]
            cap = jnp.concatenate(
                [cap_for(caps, key_block, order[b * GROUP + GATHERED[g]]) for g in blocks], axis=1
            )
            masked.append(jnp.minimum(scores[j * TOK : (j + 1) * TOK], cap))
        masked = jnp.concatenate(masked, axis=0)
        top = jnp.max(masked, axis=0, keepdims=True)
        probs = jnp.exp(masked - top).astype(BF16)
        summed = nn(kv_t[...], probs)
        grad_t = jnp.transpose(qg.astype(F32))[HD:, :]
        total = summed[2 * HD : 2 * HD + 1]
        share = 1.0 / total
        part = summed[HD : 2 * HD] * share
        dot = jnp.sum(grad_t * part, axis=0, keepdims=True)
        dprob = nt(values[...], qg)
        dscore = probs * (dprob - dot).astype(BF16)
        centred = nn(kv_t[0:HD, :], dscore) * share
        plain = summed[0:HD] * share
        rows = (*split(top + jnp.log(total)), *split(dot))
        for g in blocks:
            i = GATHERED[g]
            lanes = slice((g - first) * TOK, (g - first + 1) * TOK)
            out_ref[i, OUT : OUT + HD, :] = part[:, lanes].astype(BF16)
            out_ref[i, CENTRED : CENTRED + HD, :] = centred[:, lanes].astype(BF16)
            out_ref[i, PLAIN : PLAIN + HD, :] = plain[:, lanes].astype(BF16)
            for k, row in enumerate(rows):
                stats[k * GROUP + i : k * GROUP + i + 1, :] = row[:, lanes]
    for i in range(GROUP):
        out_ref[i, STATS:, :] = stats[...].astype(BF16)


def part_stats(parts_ref):
    logs, dots = [], []
    for p in range(GROUP):
        rows = parts_ref[p, STATS:, :].astype(F32)
        logs.append(rows[0:GROUP] + rows[GROUP : 2 * GROUP])
        dots.append(rows[2 * GROUP : 3 * GROUP] + rows[3 * GROUP :])
    return logs, dots


def joined(logs, dots):
    top = logs[0]
    for p in range(1, GROUP):
        top = jnp.maximum(top, logs[p])
    weights = [jnp.exp(logs[p] - top) for p in range(GROUP)]
    total = sum(weights)
    weights = [weight / total for weight in weights]
    dot = sum(weights[p] * dots[p] for p in range(GROUP))
    return top + jnp.log(total), dot, weights


def prepare(
    queries_hbm, kv_hbm, weight_hbm, grad_hbm, qg_ref, copies_ref, queries_t, kv, weight, grad, sems
):
    pairs = ((kv_hbm, kv), (weight_hbm, weight), (grad_hbm, grad), (queries_hbm, queries_t))
    loads = [pltpu.make_async_copy(*pair, sems.at[k]) for k, pair in enumerate(pairs)]
    for load in loads:
        load.start()
    loads[0].wait()
    for p in range(GROUP):
        copies_ref[p] = kv[...]
    for load in loads[1:]:
        load.wait()
    grad_att = nt(grad[...], weight[...])
    scaled = jnp.transpose(queries_t[...].astype(F32)) * HD**-0.5
    qg_ref[...] = jnp.concatenate([scaled, grad_att], axis=1).astype(BF16)


def join_parts(order, parts_ref, weight_ref, out_ref, own):
    a, quarter = order[A_AT], order[X_AT]
    rows = HD // QUARTERS
    _, _, weights = joined(*part_stats(parts_ref))
    for p in range(GROUP):
        own[p * GROUP : (p + 1) * GROUP, :] = weights[p]
    attended = jnp.zeros((HD, TOK), F32)
    for p in range(GROUP):
        weight = own[pl.ds(p * GROUP + a, 1), :]
        attended += weight * parts_ref[p, OUT : OUT + HD, :].astype(F32)
    out = attended.astype(BF16)
    own_rows = weight_ref[pl.ds(pl.multiple_of(quarter * rows, rows), rows), :]
    for y in range(out_ref.shape[0]):
        out_ref[y, 0:HD, :] = out
        for k in range(4):
            first = HD + k * rows
            column = (4 * y + k) * TOK
            out_ref[y, first : first + rows, :] = own_rows[:, column : column + TOK]


def mix(mixed_ref, weight_ref, out_ref, side):
    cores, chips = mixed_ref.shape[:2]
    rows = HD // QUARTERS
    for c in range(cores):
        for y in range(chips):
            for quarter in range(QUARTERS):
                first = (c * chips + y) * HD + quarter * rows
                for half in range(2):
                    side[first : first + rows, half * TOK : (half + 1) * TOK] = weight_ref[
                        quarter, c, y, half * rows : (half + 1) * rows, :
                    ]
    attended = mixed_ref[:, :, 0:HD, :].reshape(cores * chips * HD, TOK)
    out_ref[...] = lax.dot_general(
        attended, side[...], (((0,), (0,)), ((), ())), preferred_element_type=F32
    ).astype(BF16)


def backward_tile(
    order, qg_ref, kv_ref, parts_ref, dkv_ref, dq_ref, query_part, grad_part, norm_dot, caps, own
):
    b, a = order[B_AT], order[A_AT]
    logs, dots = part_stats(parts_ref)
    log_total, dot, weights = joined(logs, dots)
    for p in range(GROUP):
        scaled = weights[p] * HD**-0.5
        own[2 * p * GROUP : (2 * p + 1) * GROUP, :] = scaled
        own[(2 * p + 1) * GROUP : (2 * p + 2) * GROUP, :] = scaled * (dot - dots[p])
    dq = jnp.zeros((HD, TOK), F32)
    for p in range(GROUP):
        weight = own[pl.ds(2 * p * GROUP + a, 1), :]
        shifted = own[pl.ds((2 * p + 1) * GROUP + a, 1), :]
        dq += weight * parts_ref[p, CENTRED : CENTRED + HD, :].astype(F32)
        dq -= shifted * parts_ref[p, PLAIN : PLAIN + HD, :].astype(F32)
    dq_ref[...] = dq.astype(BF16)
    for g, i in enumerate(GATHERED):
        norm_dot[0:1, g * TOK : (g + 1) * TOK] = log_total[i : i + 1]
        norm_dot[1:2, g * TOK : (g + 1) * TOK] = dot[i : i + 1]
    qg = qg_ref[...].reshape(ROWS, 2 * HD)
    query_part[...] = lanes_below(qg)
    grad_part[...] = lanes_below(qg, True)
    fill_caps(caps)
    for j in range(GROUP):
        kv = kv_ref[j]
        key_block = order[j * GROUP + a]
        cap = jnp.concatenate(
            [cap_for(caps, key_block, order[b * GROUP + i]) for i in GATHERED], axis=1
        )
        masked = jnp.minimum(nt(kv, query_part[...]), cap)
        probs = jnp.exp(masked - norm_dot[0:1, :]).astype(BF16)
        dprob = nt(kv, grad_part[...])
        dscore = probs * (dprob - norm_dot[1:2, :]).astype(BF16)
        dkv = nn(dscore, query_part[...]) + nn(probs, grad_part[...])
        dkv_ref[j] = dkv.astype(BF16)


def smem():
    return pl.BlockSpec(memory_space=pltpu.SMEM)


def vmem():
    return pl.BlockSpec(memory_space=pltpu.VMEM)


def exchange(value, axis):
    return lax.all_to_all(value, axis, 0, 0, tiled=True)


def local(queries, keys_values, out_weight, out_grad, block_order):
    chips = lax.axis_size("y")
    heads = chips * lax.axis_size("c")
    place = [lax.axis_index(name) for name in ("b", A, "x")]
    order = jnp.concatenate([block_order, jnp.stack(place).astype(jnp.int32)])
    weight = out_weight[0]
    columns = weight.shape[1] // heads
    query_grad, kv_copies = pl.pallas_call(
        prepare,
        out_shape=(
            jax.ShapeDtypeStruct((TOK, 2 * HD), BF16),
            jax.ShapeDtypeStruct((GROUP, TOK, 2 * HD), BF16),
        ),
        in_specs=[pl.BlockSpec(memory_space=pltpu.HBM)] * 4,
        out_specs=(vmem(), vmem()),
        scratch_shapes=[
            pltpu.VMEM((HD, TOK), BF16),
            pltpu.VMEM((TOK, 2 * HD), BF16),
            pltpu.VMEM(weight.shape, BF16),
            pltpu.VMEM(out_grad.shape, BF16),
            pltpu.SemaphoreType.DMA((4,)),
        ],
        interpret=INTERPRET,
        name="prepare",
    )(jnp.transpose(queries[:, 0]), keys_values[:, 0], weight, out_grad)
    kv_group = exchange(kv_copies, "b")
    qg_group = query_grad
    for pairs in ([[0, 1], [2, 3]], [[0, 3], [1, 2]]):
        qg_group = lax.all_gather(qg_group, "x", tiled=True, axis_index_groups=pairs)
    qg_group = lax.all_gather(qg_group, "zl")
    qg_group = qg_group.reshape(GROUP, TOK, 2 * HD)
    parts = pl.pallas_call(
        forward_tile,
        out_shape=jax.ShapeDtypeStruct((GROUP, OUT_ROWS, TOK), BF16),
        in_specs=[smem(), vmem(), vmem()],
        out_specs=vmem(),
        scratch_shapes=[
            pltpu.VMEM((ROWS, 2 * HD), BF16),
            pltpu.VMEM((ROWS, 2 * HD), BF16),
            pltpu.VMEM((2 * HD + 16, ROWS), BF16),
            pltpu.VMEM((STAT_ROWS, TOK), F32),
            pltpu.VMEM((3 * TOK, TOK), F32),
        ],
        interpret=INTERPRET,
        compiler_params=PARAMS,
        name="forward_tile",
    )(order, qg_group, kv_group)
    parts = exchange(parts, A)
    mixed_parts = pl.pallas_call(
        join_parts,
        out_shape=jax.ShapeDtypeStruct((chips, 2 * HD, TOK), BF16),
        in_specs=[smem(), vmem(), vmem()],
        out_specs=vmem(),
        scratch_shapes=[pltpu.VMEM((GROUP * GROUP, TOK), F32)],
        interpret=INTERPRET,
        compiler_params=PARAMS,
        name="join_parts",
    )(order, parts, weight)
    mixed_parts = exchange(mixed_parts, "y")
    every_head = lax.all_gather(mixed_parts, "c")
    own_side = 2 * HD // QUARTERS
    quarters = lax.dynamic_slice_in_dim(
        every_head, HD + lax.axis_index("c") * own_side, own_side, axis=2
    )
    quarters = lax.all_gather(quarters, "x")
    mixed_out = pl.pallas_call(
        mix,
        out_shape=jax.ShapeDtypeStruct((TOK, columns), BF16),
        in_specs=[vmem(), vmem()],
        out_specs=vmem(),
        scratch_shapes=[pltpu.VMEM((heads * HD, columns), BF16)],
        interpret=INTERPRET,
        compiler_params=PARAMS,
        name="mix",
    )(every_head, quarters)
    dkv, grad_queries = pl.pallas_call(
        backward_tile,
        out_shape=(
            jax.ShapeDtypeStruct((GROUP, TOK, 2 * HD), BF16),
            jax.ShapeDtypeStruct((HD, TOK), BF16),
        ),
        in_specs=[smem(), vmem(), vmem(), vmem()],
        out_specs=(vmem(), vmem()),
        scratch_shapes=[
            pltpu.VMEM((ROWS, 2 * HD), BF16),
            pltpu.VMEM((ROWS, 2 * HD), BF16),
            pltpu.VMEM((8, ROWS), F32),
            pltpu.VMEM((3 * TOK, TOK), F32),
            pltpu.VMEM((2 * GROUP * GROUP, TOK), F32),
        ],
        interpret=INTERPRET,
        compiler_params=PARAMS,
        name="backward_tile",
    )(order, qg_group, kv_group, parts)
    dkv = exchange(dkv, "b")
    grad_keys_values = jnp.sum(dkv.astype(F32), axis=0).astype(BF16)[:, None]
    return (mixed_out, jnp.transpose(grad_queries)[:, None], grad_keys_values)


def solution(mesh):
    finer = Mesh(mesh.devices.reshape(GROUP, 2, 4, mesh.shape["head"] // 2, 2), (*SEQ, *HEAD))
    in_specs = (
        P(SEQ, HEAD, None),
        P(SEQ, HEAD, None),
        P(HEAD, None, None),
        P(SEQ, None),
        P(),
    )
    out_specs = (P(SEQ, HEAD), P(SEQ, HEAD, None), P(SEQ, HEAD, None))
    return jax.shard_map(local, mesh=finer, in_specs=in_specs, out_specs=out_specs, check_vma=False)
```

```python
import jax
import jax.numpy as jnp
from jax import lax
from jax.experimental import pallas as pl
from jax.experimental.pallas import tpu as pltpu
from jax.sharding import Mesh
from jax.sharding import PartitionSpec as P

GROUP = 8
SEQ = ("b", "zl", "x")
TOK = 128
HD = 64
ROWS = GROUP * TOK
OUT, CENTRED, PLAIN, STATS = 0, HD, 2 * HD, 3 * HD
STAT_ROWS = 32
OUT_ROWS = STATS + STAT_ROWS
QUARTERS = 4
PIECES = 2
WIDE = 8
A = ("zl", "x")
HEAD = ("y", "c")
GATHERED = range(GROUP)
B_AT, A_AT, X_AT = 64, 65, 66
NEG = -(2.0**100)
INTERPRET = False
PARAMS = pltpu.CompilerParams(vmem_limit_bytes=24 * 1024 * 1024)
F32 = jnp.float32
BF16 = jnp.bfloat16


def nt(x, y):
    return lax.dot_general(x, y, (((1,), (1,)), ((), ())), preferred_element_type=F32)


def nn(x, y):
    return lax.dot_general(x, y, (((1,), (0,)), ((), ())), preferred_element_type=F32)


def lanes_below(x, flip=False):
    lane = lax.broadcasted_iota(jnp.int32, x.shape, x.ndim - 1)
    keep = lane >= HD if flip else lane < HD
    return jnp.where(keep, x, jnp.zeros_like(x))


def fill_caps(caps):
    key = lax.broadcasted_iota(jnp.int32, (TOK, TOK), 0)
    query = lax.broadcasted_iota(jnp.int32, (TOK, TOK), 1)
    caps[0:TOK, :] = jnp.full((TOK, TOK), NEG, F32)
    caps[TOK : 2 * TOK, :] = jnp.where(key <= query, -NEG, NEG)
    caps[2 * TOK :, :] = jnp.full((TOK, TOK), -NEG, F32)


def cap_for(caps, key_block, query_block):
    later = jnp.clip(query_block - key_block, -1, 1) + 1
    return caps[pl.ds(pl.multiple_of(later * TOK, TOK), TOK), :]


def split(value):
    high = value.astype(BF16).astype(F32)
    return high, value - high


def forward_tile(order, qg_ref, kv_ref, out_ref, keys, values, kv_t, stats, caps):
    b, a = order[B_AT], order[A_AT]
    kv = kv_ref[...].reshape(ROWS, 2 * HD)
    keys[...] = lanes_below(kv)
    values[...] = lanes_below(kv, True)
    kv_t[0 : 2 * HD, :] = jnp.transpose(kv.astype(F32)).astype(BF16)
    kv_t[2 * HD :, :] = jnp.ones((16, ROWS), BF16)
    stats[...] = jnp.zeros((STAT_ROWS, TOK), F32)
    fill_caps(caps)
    for first in range(0, GROUP, WIDE):
        blocks = range(first, first + WIDE)
        qg = qg_ref[first : first + WIDE].reshape(WIDE * TOK, 2 * HD)
        scores = nt(keys[...], qg)
        masked = []
        for j in range(GROUP):
            key_block = order[j * GROUP + a]
            cap = jnp.concatenate(
                [cap_for(caps, key_block, order[b * GROUP + GATHERED[g]]) for g in blocks], axis=1
            )
            masked.append(jnp.minimum(scores[j * TOK : (j + 1) * TOK], cap))
        masked = jnp.concatenate(masked, axis=0)
        top = jnp.max(masked, axis=0, keepdims=True)
        probs = jnp.exp(masked - top).astype(BF16)
        summed = nn(kv_t[...], probs)
        grad_t = jnp.transpose(qg.astype(F32))[HD:, :]
        total = summed[2 * HD : 2 * HD + 1]
        share = 1.0 / total
        part = summed[HD : 2 * HD] * share
        dot = jnp.sum(grad_t * part, axis=0, keepdims=True)
        dprob = nt(values[...], qg)
        dscore = probs * (dprob - dot).astype(BF16)
        centred = nn(kv_t[0:HD, :], dscore) * share
        plain = summed[0:HD] * share
        rows = (*split(top + jnp.log(total)), *split(dot))
        for g in blocks:
            i = GATHERED[g]
            lanes = slice((g - first) * TOK, (g - first + 1) * TOK)
            out_ref[i, OUT : OUT + HD, :] = part[:, lanes].astype(BF16)
            out_ref[i, CENTRED : CENTRED + HD, :] = centred[:, lanes].astype(BF16)
            out_ref[i, PLAIN : PLAIN + HD, :] = plain[:, lanes].astype(BF16)
            for k, row in enumerate(rows):
                stats[k * GROUP + i : k * GROUP + i + 1, :] = row[:, lanes]
    for i in range(GROUP):
        out_ref[i, STATS:, :] = stats[...].astype(BF16)


def part_stats(parts_ref):
    logs, dots = [], []
    for p in range(GROUP):
        rows = parts_ref[p, STATS:, :].astype(F32)
        logs.append(rows[0:GROUP] + rows[GROUP : 2 * GROUP])
        dots.append(rows[2 * GROUP : 3 * GROUP] + rows[3 * GROUP :])
    return logs, dots


def joined(logs, dots):
    top = logs[0]
    for p in range(1, GROUP):
        top = jnp.maximum(top, logs[p])
    weights = [jnp.exp(logs[p] - top) for p in range(GROUP)]
    total = sum(weights)
    weights = [weight / total for weight in weights]
    dot = sum(weights[p] * dots[p] for p in range(GROUP))
    return top + jnp.log(total), dot, weights


def prepare(
    queries_hbm, kv_hbm, weight_hbm, grad_hbm, qg_ref, copies_hbm, queries_t, weight, grad, sems
):
    spread = [
        pltpu.make_async_copy(kv_hbm, copies_hbm.at[p], sems.at[p]) for p in range(GROUP)
    ]
    width = weight.shape[1] // PIECES
    pieces = [pl.ds(k * width, width) for k in range(PIECES)]
    pairs = [(queries_hbm, queries_t)]
    for piece in pieces:
        pairs.append((weight_hbm.at[:, piece], weight.at[:, piece]))
        pairs.append((grad_hbm.at[:, piece], grad.at[:, piece]))
    loads = [pltpu.make_async_copy(*pair, sems.at[GROUP + k]) for k, pair in enumerate(pairs)]
    for copy in spread + loads:
        copy.start()
    loads[0].wait()
    scaled = jnp.transpose(queries_t[...].astype(F32)) * HD**-0.5
    grad_att = jnp.zeros((TOK, HD), F32)
    for k, piece in enumerate(pieces):
        loads[1 + 2 * k].wait()
        loads[2 + 2 * k].wait()
        grad_att += nt(grad[:, piece], weight[:, piece])
    qg_ref[...] = jnp.concatenate([scaled, grad_att], axis=1).astype(BF16)
    for copy in spread:
        copy.wait()


def join_parts(order, parts_ref, weight_ref, out_ref, own):
    a, quarter = order[A_AT], order[X_AT]
    rows = HD // QUARTERS
    _, _, weights = joined(*part_stats(parts_ref))
    for p in range(GROUP):
        own[p * GROUP : (p + 1) * GROUP, :] = weights[p]
    attended = jnp.zeros((HD, TOK), F32)
    for p in range(GROUP):
        weight = own[pl.ds(p * GROUP + a, 1), :]
        attended += weight * parts_ref[p, OUT : OUT + HD, :].astype(F32)
    out = attended.astype(BF16)
    own_rows = weight_ref[pl.ds(pl.multiple_of(quarter * rows, rows), rows), :]
    for y in range(out_ref.shape[0]):
        out_ref[y, 0:HD, :] = out
        for k in range(4):
            first = HD + k * rows
            column = (4 * y + k) * TOK
            out_ref[y, first : first + rows, :] = own_rows[:, column : column + TOK]


def mix(mixed_ref, weight_ref, out_ref, side):
    cores, chips = mixed_ref.shape[:2]
    rows = HD // QUARTERS
    for c in range(cores):
        for y in range(chips):
            for quarter in range(QUARTERS):
                first = (c * chips + y) * HD + quarter * rows
                for half in range(2):
                    side[first : first + rows, half * TOK : (half + 1) * TOK] = weight_ref[
                        quarter, c, y, half * rows : (half + 1) * rows, :
                    ]
    attended = mixed_ref[:, :, 0:HD, :].reshape(cores * chips * HD, TOK)
    out_ref[...] = lax.dot_general(
        attended, side[...], (((0,), (0,)), ((), ())), preferred_element_type=F32
    ).astype(BF16)


def backward_tile(
    order, qg_ref, kv_ref, parts_ref, dkv_ref, dq_ref, query_part, grad_part, norm_dot, caps, own
):
    b, a = order[B_AT], order[A_AT]
    logs, dots = part_stats(parts_ref)
    log_total, dot, weights = joined(logs, dots)
    for p in range(GROUP):
        scaled = weights[p] * HD**-0.5
        own[2 * p * GROUP : (2 * p + 1) * GROUP, :] = scaled
        own[(2 * p + 1) * GROUP : (2 * p + 2) * GROUP, :] = scaled * (dot - dots[p])
    dq = jnp.zeros((HD, TOK), F32)
    for p in range(GROUP):
        weight = own[pl.ds(2 * p * GROUP + a, 1), :]
        shifted = own[pl.ds((2 * p + 1) * GROUP + a, 1), :]
        dq += weight * parts_ref[p, CENTRED : CENTRED + HD, :].astype(F32)
        dq -= shifted * parts_ref[p, PLAIN : PLAIN + HD, :].astype(F32)
    dq_ref[...] = dq.astype(BF16)
    for g, i in enumerate(GATHERED):
        norm_dot[0:1, g * TOK : (g + 1) * TOK] = log_total[i : i + 1]
        norm_dot[1:2, g * TOK : (g + 1) * TOK] = dot[i : i + 1]
    qg = qg_ref[...].reshape(ROWS, 2 * HD)
    query_part[...] = lanes_below(qg)
    grad_part[...] = lanes_below(qg, True)
    fill_caps(caps)
    for j in range(GROUP):
        kv = kv_ref[j]
        key_block = order[j * GROUP + a]
        cap = jnp.concatenate(
            [cap_for(caps, key_block, order[b * GROUP + i]) for i in GATHERED], axis=1
        )
        masked = jnp.minimum(nt(kv, query_part[...]), cap)
        probs = jnp.exp(masked - norm_dot[0:1, :]).astype(BF16)
        dprob = nt(kv, grad_part[...])
        dscore = probs * (dprob - norm_dot[1:2, :]).astype(BF16)
        dkv = nn(dscore, query_part[...]) + nn(probs, grad_part[...])
        dkv_ref[j] = dkv.astype(BF16)


def smem():
    return pl.BlockSpec(memory_space=pltpu.SMEM)


def vmem():
    return pl.BlockSpec(memory_space=pltpu.VMEM)


def exchange(value, axis):
    return lax.all_to_all(value, axis, 0, 0, tiled=True)


def local(queries, keys_values, out_weight, out_grad, block_order):
    chips = lax.axis_size("y")
    heads = chips * lax.axis_size("c")
    place = [lax.axis_index(name) for name in ("b", A, "x")]
    order = jnp.concatenate([block_order, jnp.stack(place).astype(jnp.int32)])
    weight = out_weight[0]
    columns = weight.shape[1] // heads
    query_grad, kv_copies = pl.pallas_call(
        prepare,
        out_shape=(
            jax.ShapeDtypeStruct((TOK, 2 * HD), BF16),
            jax.ShapeDtypeStruct((GROUP, TOK, 2 * HD), BF16),
        ),
        in_specs=[pl.BlockSpec(memory_space=pltpu.HBM)] * 4,
        out_specs=(vmem(), pl.BlockSpec(memory_space=pltpu.HBM)),
        scratch_shapes=[
            pltpu.VMEM((HD, TOK), BF16),
            pltpu.VMEM(weight.shape, BF16),
            pltpu.VMEM(out_grad.shape, BF16),
            pltpu.SemaphoreType.DMA((GROUP + 1 + 2 * PIECES,)),
        ],
        interpret=INTERPRET,
        name="prepare",
    )(jnp.transpose(queries[:, 0]), keys_values[:, 0], weight, out_grad)
    kv_group = exchange(kv_copies, "b")
    qg_group = query_grad
    for pairs in ([[0, 1], [2, 3]], [[0, 3], [1, 2]]):
        qg_group = lax.all_gather(qg_group, "x", tiled=True, axis_index_groups=pairs)
    qg_group = lax.all_gather(qg_group, "zl")
    qg_group = qg_group.reshape(GROUP, TOK, 2 * HD)
    parts = pl.pallas_call(
        forward_tile,
        out_shape=jax.ShapeDtypeStruct((GROUP, OUT_ROWS, TOK), BF16),
        in_specs=[smem(), vmem(), vmem()],
        out_specs=vmem(),
        scratch_shapes=[
            pltpu.VMEM((ROWS, 2 * HD), BF16),
            pltpu.VMEM((ROWS, 2 * HD), BF16),
            pltpu.VMEM((2 * HD + 16, ROWS), BF16),
            pltpu.VMEM((STAT_ROWS, TOK), F32),
            pltpu.VMEM((3 * TOK, TOK), F32),
        ],
        interpret=INTERPRET,
        compiler_params=PARAMS,
        name="forward_tile",
    )(order, qg_group, kv_group)
    parts = exchange(parts, A)
    mixed_parts = pl.pallas_call(
        join_parts,
        out_shape=jax.ShapeDtypeStruct((chips, 2 * HD, TOK), BF16),
        in_specs=[smem(), vmem(), vmem()],
        out_specs=vmem(),
        scratch_shapes=[pltpu.VMEM((GROUP * GROUP, TOK), F32)],
        interpret=INTERPRET,
        compiler_params=PARAMS,
        name="join_parts",
    )(order, parts, weight)
    mixed_parts = exchange(mixed_parts, "y")
    every_head = lax.all_gather(mixed_parts, "c")
    own_side = 2 * HD // QUARTERS
    quarters = lax.dynamic_slice_in_dim(
        every_head, HD + lax.axis_index("c") * own_side, own_side, axis=2
    )
    quarters = lax.all_gather(quarters, "x")
    mixed_out = pl.pallas_call(
        mix,
        out_shape=jax.ShapeDtypeStruct((TOK, columns), BF16),
        in_specs=[vmem(), vmem()],
        out_specs=vmem(),
        scratch_shapes=[pltpu.VMEM((heads * HD, columns), BF16)],
        interpret=INTERPRET,
        compiler_params=PARAMS,
        name="mix",
    )(every_head, quarters)
    dkv, grad_queries = pl.pallas_call(
        backward_tile,
        out_shape=(
            jax.ShapeDtypeStruct((GROUP, TOK, 2 * HD), BF16),
            jax.ShapeDtypeStruct((HD, TOK), BF16),
        ),
        in_specs=[smem(), vmem(), vmem(), vmem()],
        out_specs=(vmem(), vmem()),
        scratch_shapes=[
            pltpu.VMEM((ROWS, 2 * HD), BF16),
            pltpu.VMEM((ROWS, 2 * HD), BF16),
            pltpu.VMEM((8, ROWS), F32),
            pltpu.VMEM((3 * TOK, TOK), F32),
            pltpu.VMEM((2 * GROUP * GROUP, TOK), F32),
        ],
        interpret=INTERPRET,
        compiler_params=PARAMS,
        name="backward_tile",
    )(order, qg_group, kv_group, parts)
    dkv = exchange(dkv, "b")
    grad_keys_values = jnp.sum(dkv.astype(F32), axis=0).astype(BF16)[:, None]
    return (mixed_out, jnp.transpose(grad_queries)[:, None], grad_keys_values)


def solution(mesh):
    finer = Mesh(mesh.devices.reshape(GROUP, 2, 4, mesh.shape["head"] // 2, 2), (*SEQ, *HEAD))
    in_specs = (
        P(SEQ, HEAD, None),
        P(SEQ, HEAD, None),
        P(HEAD, None, None),
        P(SEQ, None),
        P(),
    )
    out_specs = (P(SEQ, HEAD), P(SEQ, HEAD, None), P(SEQ, HEAD, None))
    return jax.shard_map(local, mesh=finer, in_specs=in_specs, out_specs=out_specs, check_vma=False)
```
